32 devices in a mesh: tiles: 16 (over z, x, core), strip: 2 (over y).
Axes of the slice: x: 2, y: 2, z: 4, core: 2. Of those that a mesh axis runs over, the one named last changes fastest.
Arguments:
- fields: float32 [16, 2, 3, 3, 4, 8100], P('tiles', 'strip'), may hold values from -6 to 6
- wet_land: int32 [16, 2, 3, 8100], P('tiles', 'strip'), may hold values from 0 to 1, as said below
- links: int32 [16, 2, 3, 4, 4], P('tiles', 'strip'), may hold values from -1 to 3, as said below
- surface_diagonal: float32 [16, 2, 3, 8100], P('tiles', 'strip'), may hold values from 0.25 to 2
- spread: float32 [3, 4], replicated, may hold values from 0.02 to 0.2
- mixing: float32 [4], replicated, may hold values from 0.02 to 0.2
- thickness: float32 [4], replicated, may hold values from 0.5 to 2
Outputs:
- adjoint_fields: float32 [16, 2, 3, 3, 4, 8100], P('tiles', 'strip')
- surface_solution: float32 [16, 2, 3, 8100], P('tiles', 'strip')
- surface_residual: float32 [16, 2, 3, 8100], P('tiles', 'strip')
The draws below stay inside these ranges and needn't reach their ends.
Inputs may be any that keep to these rules, and one draw needn't show every extreme that they name: wet_land is 1 on most cells of the first 1 to 3 slots of each device and 0 on all cells of its other slots. Offsets dt and ds are -1, 0 or 1; on the west and east sides dt is -1 and 1, on the south and north sides ds is -1 and 1; a partner slot is -1 or a slot that holds wet cells; links are mutual: side e of slot k pairs with side e XOR 1 of its partner, whose entry points back with opposite offsets and rotation code (4 - code) mod 4; an empty slot has no links; rotation codes are 0 to 3.
All inputs are finite; a program needn't handle non-finite values.
Results may differ from the reference program's by a relative error of at most 0.00027.
Values sent between devices are 32-bit elements; how exact they have to be, the bound alone decides.
No kernel may reach another device: no remote copies, remote signals or barrier semaphores. Data moves between devices by JAX's collectives and lax.ppermute only.
A program may use at most 64 MiB of HBM per device.

```python
import math
import jax
import jax.numpy as jnp
import numpy as np
from jax import lax

TILE = 90
SLOTS = 3
FIELDS = 3
LEVELS = 4
ITERS = 2
CELLS = 8100
TILE_GROUPS = 16
STRIP_GROUPS = 2


def wet_counts(key):
    return jax.random.randint(jax.random.fold_in(key, 11), (TILE_GROUPS, STRIP_GROUPS), 1, SLOTS + 1)


def live_slots(key):
    counts = wet_counts(key)
    return jnp.arange(SLOTS, dtype=jnp.int32)[None, None, :] < counts[:, :, None]


def draw_wet_land(key, part):
    live = live_slots(key)
    ocean = jax.random.randint(jax.random.fold_in(key, 13), (TILE_GROUPS, STRIP_GROUPS, SLOTS, CELLS), 0, 8) != 0
    return (live[..., None] & ocean).astype(jnp.int32)


def slot_orders(key):
    scores = jax.random.randint(key, (TILE_GROUPS, STRIP_GROUPS, SLOTS), 0, 1 << 20) * SLOTS
    scores = scores + jnp.arange(SLOTS, dtype=jnp.int32)[None, None, :]
    order = jnp.argsort(scores, axis=-1).astype(jnp.int32)
    inverse = jnp.argsort(order, axis=-1).astype(jnp.int32)
    return (order, inverse)


def entry_table(group_shift, strip_shift, partner, code):
    shape = (TILE_GROUPS, STRIP_GROUPS, SLOTS)
    return jnp.stack([jnp.broadcast_to(group_shift, shape), jnp.broadcast_to(strip_shift, shape), jnp.broadcast_to(partner, shape), jnp.broadcast_to(code, shape)], axis=-1).astype(jnp.int32)


def draw_links(key, part):
    live = live_slots(key)
    shape = (TILE_GROUPS, STRIP_GROUPS, SLOTS)
    group_ids = jnp.arange(TILE_GROUPS, dtype=jnp.int32)[:, None, None]
    strip_ids = jnp.arange(STRIP_GROUPS, dtype=jnp.int32)[None, :, None]
    slot_ids = jnp.arange(SLOTS, dtype=jnp.int32)[None, None, :]
    east_shift = jax.random.randint(jax.random.fold_in(key, 21), (TILE_GROUPS,), -1, 2)
    east_order, east_inverse = slot_orders(jax.random.fold_in(key, 22))
    east_code = jax.random.randint(jax.random.fold_in(key, 23), shape, 0, 4)
    east_cut = jax.random.randint(jax.random.fold_in(key, 24), shape, 0, 8) == 0
    east_group = (group_ids + 1) % TILE_GROUPS
    east_strip = (strip_ids + east_shift[:, None, None]) % STRIP_GROUPS
    east_live = live & live[east_group, east_strip, east_order] & jnp.logical_not(east_cut)
    east_entry = entry_table(1, east_shift[:, None, None], jnp.where(east_live, east_order, -1), east_code)
    from_group = (group_ids - 1) % TILE_GROUPS
    west_shift = east_shift[from_group]
    from_strip = (strip_ids - west_shift) % STRIP_GROUPS
    from_slot = east_inverse[from_group, from_strip, slot_ids]
    west_live = east_live[from_group, from_strip, from_slot]
    west_code = (4 - east_code[from_group, from_strip, from_slot]) % 4
    west_entry = entry_table(-1, -west_shift, jnp.where(west_live, from_slot, -1), west_code)
    north_shift = jax.random.randint(jax.random.fold_in(key, 31), (STRIP_GROUPS,), -1, 2)
    north_order, north_inverse = slot_orders(jax.random.fold_in(key, 32))
    north_code = jax.random.randint(jax.random.fold_in(key, 33), shape, 0, 4)
    north_cut = jax.random.randint(jax.random.fold_in(key, 34), shape, 0, 8) == 0
    north_group = (group_ids + north_shift[None, :, None]) % TILE_GROUPS
    north_strip = (strip_ids + 1) % STRIP_GROUPS
    north_live = live & live[north_group, north_strip, north_order] & jnp.logical_not(north_cut)
    north_entry = entry_table(north_shift[None, :, None], 1, jnp.where(north_live, north_order, -1), north_code)
    below_strip = (strip_ids - 1) % STRIP_GROUPS
    south_shift = north_shift[below_strip]
    below_group = (group_ids - south_shift) % TILE_GROUPS
    below_slot = north_inverse[below_group, below_strip, slot_ids]
    south_live = north_live[below_group, below_strip, below_slot]
    south_code = (4 - north_code[below_group, below_strip, below_slot]) % 4
    south_entry = entry_table(-south_shift, -1, jnp.where(south_live, below_slot, -1), south_code)
    return jnp.stack([west_entry, east_entry, south_entry, north_entry], axis=3)


def steps_of(stream_key, dims, cuts, low, largest):
    def one(position, blocks):
        draws = jax.random.uniform(jax.random.fold_in(jax.random.fold_in(stream_key, 6), position), (blocks,), jnp.float32, low / len(cuts), largest / len(cuts))
        return jnp.repeat(jnp.exp(draws), dims[position] // blocks).reshape((-1,) + (1,) * (len(dims) - position - 1))

    level = one(*cuts[0])
    for cut in cuts[1:]:
        level = level * one(*cut)
    return level


def scatter_about(key, extent, scale, bound, cuts=(), kind=jnp.bfloat16):
    gain = steps_of(key, extent, cuts, -0.22, 0.18) if cuts else 1.0
    values = jax.random.normal(key, extent, jnp.float32) * scale * gain
    return jnp.minimum(jnp.maximum(values, -bound), bound).astype(kind)


def setup_inputs(seed: int = 0) -> dict:
    key_list = jax.random.split(jax.random.key(seed), 8)
    return {
        "fields": scatter_about(key_list[0], (TILE_GROUPS, STRIP_GROUPS, SLOTS, FIELDS, LEVELS, CELLS), 1.0, 6.0, ((0, 16), (1, 2)), jnp.float32),
        "wet_land": draw_wet_land(jax.random.fold_in(key_list[7], 71), 0),
        "links": draw_links(jax.random.fold_in(key_list[7], 71), 0),
        "surface_diagonal": jnp.clip(0.25 + 1.75 * jax.random.uniform(key_list[3], (TILE_GROUPS, STRIP_GROUPS, SLOTS, CELLS), jnp.float32) ** steps_of(key_list[3], (TILE_GROUPS, STRIP_GROUPS, SLOTS, CELLS), ((0, 16), (1, 2)), -0.2, 0.2), 0.25, 2.0),
        "spread": jnp.clip(jnp.exp(jax.random.uniform(key_list[4], (FIELDS, LEVELS), jnp.float32, math.log(0.02), math.log(0.2))), 0.02, 0.2),
        "mixing": jnp.clip(jnp.exp(jax.random.uniform(key_list[5], (LEVELS,), jnp.float32, math.log(0.02), math.log(0.2))), 0.02, 0.2),
        "thickness": jnp.clip(jnp.exp(jax.random.uniform(key_list[6], (LEVELS,), jnp.float32, math.log(0.5), math.log(2.0))), 0.5, 2.0),
    }


OPPOSITE = np.array([1, 0, 3, 2], np.int32)


def rim_rows(values, width):
    west_rim = values[..., ::width]
    east_rim = values[..., width - 1::width]
    south_rim = values[..., :width]
    north_rim = values[..., -width:]
    return jnp.concatenate([west_rim, east_rim, south_rim, north_rim], axis=-1)


def beside_values(values, rims, width):
    cells_total = values.shape[-1]
    leading = values.shape[:-1]
    places = jnp.arange(cells_total, dtype=jnp.int32)
    column_index = places % width
    row_index = places // width
    west_full = jnp.broadcast_to(rims[..., 0, :, None], leading + (width, width)).reshape(leading + (cells_total,))
    east_full = jnp.broadcast_to(rims[..., 1, :, None], leading + (width, width)).reshape(leading + (cells_total,))
    south_full = jnp.broadcast_to(rims[..., 2, None, :], leading + (width, width)).reshape(leading + (cells_total,))
    north_full = jnp.broadcast_to(rims[..., 3, None, :], leading + (width, width)).reshape(leading + (cells_total,))
    zero_cell = jnp.zeros(leading + (1,), jnp.float32)
    zero_line = jnp.zeros(leading + (width,), jnp.float32)
    west_side = jnp.where(column_index == 0, west_full, jnp.concatenate([zero_cell, values[..., :-1]], -1))
    east_side = jnp.where(column_index == width - 1, east_full, jnp.concatenate([values[..., 1:], zero_cell], -1))
    south_side = jnp.where(row_index == 0, south_full, jnp.concatenate([zero_line, values[..., :-width]], -1))
    north_side = jnp.where(row_index == width - 1, north_full, jnp.concatenate([values[..., width:], zero_line], -1))
    return west_side, east_side, south_side, north_side


def orient(picked, links, vector):
    code = links[..., 3]
    partner = links[..., 2]
    lead = code.ndim
    extra = picked.ndim - lead
    tail_shape = code.shape + (1,) * extra
    flipped = jnp.where((code != 0).reshape(tail_shape), jnp.flip(picked, -1), picked)
    flipped = flipped * (partner >= 0).astype(jnp.float32).reshape(tail_shape)
    if vector:
        turn_shape = code.shape + (1,) * (extra - 1)
        cosine_part = ((code == 0).astype(jnp.float32) - (code == 2).astype(jnp.float32)).reshape(turn_shape)
        sine_part = ((code == 1).astype(jnp.float32) - (code == 3).astype(jnp.float32)).reshape(turn_shape)
        eastward = jnp.take(flipped, 0, axis=lead)
        northward = jnp.take(flipped, 1, axis=lead)
        scalar_part = jnp.take(flipped, 2, axis=lead)
        flipped = jnp.stack([cosine_part * eastward + sine_part * northward,
                             cosine_part * northward - sine_part * eastward, scalar_part], axis=lead)
    return jnp.moveaxis(flipped, lead - 1, -2)


def slab_step(fields, wet, rims, spread, mixing, thickness, width):
    wet_cells = wet[..., None, None, :]
    masked = fields * wet_cells
    west_side, east_side, south_side, north_side = beside_values(masked, rims, width)
    flat_term = west_side + east_side + south_side + north_side - 4.0 * masked
    above = jnp.concatenate([masked[..., 1:, :], masked[..., -1:, :]], axis=-2)
    below = jnp.concatenate([masked[..., :1, :], masked[..., :-1, :]], axis=-2)
    column_term = above + below - 2.0 * masked
    updated = wet_cells * (masked + spread[:, :, None] * flat_term + mixing[:, None] * column_term)
    flux = 0.5 * (east_side[..., 0, :, :] - west_side[..., 0, :, :] + north_side[..., 1, :, :] - south_side[..., 1, :, :])
    source = wet * jnp.sum(thickness[:, None] * flux, axis=-2)
    return updated, source


def surface_apply(values, wet, rims, diagonal, width):
    west_side, east_side, south_side, north_side = beside_values(values, rims, width)
    return wet * ((4.0 + diagonal) * values - (west_side + east_side + south_side + north_side))


def pick_global(packs, links):
    group_shift = links[..., 0]
    strip_shift = links[..., 1]
    partner = jnp.maximum(links[..., 2], 0)
    group_index = (jnp.arange(TILE_GROUPS, dtype=jnp.int32)[:, None, None, None] + group_shift) % TILE_GROUPS
    strip_index = (jnp.arange(STRIP_GROUPS, dtype=jnp.int32)[None, :, None, None] + strip_shift) % STRIP_GROUPS
    opposite = jnp.broadcast_to(jnp.asarray(OPPOSITE)[None, None, None, :], partner.shape)
    return packs[group_index, strip_index, partner, ..., opposite, :]


def reference(fields, wet_land, links, surface_diagonal, spread, mixing, thickness):
    wet = wet_land.astype(jnp.float32)
    masked = fields * wet[:, :, :, None, None, :]
    slab_packs = rim_rows(masked, TILE).reshape(masked.shape[:-1] + (4, TILE))
    slab_rims = orient(pick_global(slab_packs, links), links, True)

    def one_group(items):
        group_fields, group_wet, group_rims = items
        return slab_step(group_fields, group_wet, group_rims, spread, mixing, thickness, TILE)

    updated, source = lax.map(one_group, (fields, wet, slab_rims))

    def surface_image(values):
        packs = rim_rows(values, TILE).reshape(values.shape[:-1] + (4, TILE))
        rims = orient(pick_global(packs, links), links, False)
        return surface_apply(values, wet, rims, surface_diagonal, TILE)

    solution = jnp.zeros_like(source)
    residual = source
    direction = source
    norm_now = jnp.sum(residual * residual)
    for iteration in range(ITERS):
        image = surface_image(direction)
        alpha = norm_now / jnp.sum(direction * image)
        solution = solution + alpha * direction
        residual = residual - alpha * image
        if iteration + 1 < ITERS:
            norm_next = jnp.sum(residual * residual)
            direction = residual + (norm_next / norm_now) * direction
            norm_now = norm_next
    return updated, solution, residual
```

```python
import functools
import math

import jax
import jax.numpy as jnp
from jax import lax
from jax.experimental import pallas as pl
from jax.experimental.pallas import tpu as pltpu
from jax.sharding import PartitionSpec as P

LANES = 128
SUBLANES = 8
ENDS = 8
F32 = jnp.float32
VMEM = pl.BlockSpec(memory_space=pltpu.VMEM)
SMEM = pl.BlockSpec(memory_space=pltpu.SMEM)


def lanes_of(rows):
    return lax.broadcasted_iota(jnp.int32, (rows, LANES), 1)


def rows_of(rows):
    return lax.broadcasted_iota(jnp.int32, (rows, LANES), 0)


def turn(value, shift):
    shift %= LANES
    return value if shift == 0 else pltpu.roll(value, shift, 1)


def take_lanes(value, index):
    return jnp.take_along_axis(value, index, axis=1, mode="promise_in_bounds")


def tile_count(cells):
    return -(-cells // LANES)


def tile_lanes(cells, tile):
    return min(LANES, cells - tile * LANES)


def seams(width, tile):
    found = []
    for b in range(width + 1):
        place = b * width
        west = b < width and place // LANES == tile
        east = b > 0 and (place - 1) // LANES == tile
        if west or east:
            found.append((b, place, west, east))
    return found


def edge_lines(tile_of, rows, width):
    cells = width * width
    lane = lanes_of(rows)
    west = east = jnp.zeros((rows, LANES), F32)
    for t in range(tile_count(cells)):
        values = tile_of(t)
        for b, place, is_west, is_east in seams(width, t):
            rolled = turn(values, b - place)
            if is_west:
                west = jnp.where(lane == b, rolled, west)
            if is_east:
                east = jnp.where(lane == b - 1, rolled, east)
    south = jnp.where(lane < width, tile_of(0), 0.0)
    start = cells - width
    t, skip = divmod(start, LANES)
    north = turn(tile_of(t), -skip)
    if skip + width > LANES:
        north = jnp.where(lane < LANES - skip, north, turn(tile_of(t + 1), -skip))
    north = jnp.where(lane < width, north, 0.0)
    return west, east, south, north


def pack_kernel(width, field_ref, wet_ref, diag_ref, pack_ref, tail_ref):
    _, fields, levels, cells = field_ref.shape
    last = tile_count(cells) - 1
    keep = tile_lanes(cells, last)
    tail_ref[...] = jnp.zeros_like(tail_ref)
    for f in range(fields):
        tail_ref[f * levels : (f + 1) * levels, :keep] = field_ref[0, f, :, last * LANES : cells]
    base = fields * levels
    tail_ref[base : base + 1, :keep] = wet_ref[0, :, last * LANES : cells].astype(F32)
    tail_ref[base + 1 : base + 2, :keep] = diag_ref[0, :, last * LANES : cells]

    def field_tile(f, t):
        if t == last:
            return tail_ref[f * levels : (f + 1) * levels, :]
        return field_ref[0, f, :, t * LANES : (t + 1) * LANES]

    def wet_tile(t):
        if t == last:
            return tail_ref[base : base + 1, :]
        return wet_ref[0, :, t * LANES : (t + 1) * LANES].astype(F32)

    def diag_tile(t):
        if t == last:
            return tail_ref[base + 1 : base + 2, :]
        return diag_ref[0, :, t * LANES : (t + 1) * LANES]

    wet_lines = edge_lines(wet_tile, 1, width)
    diag_lines = edge_lines(diag_tile, 1, width)
    for e in range(4):
        pack_ref[e, 0, base : base + 1, :] = wet_lines[e]
        pack_ref[e, 0, base + 1 : base + 2, :] = diag_lines[e]
        pack_ref[e, 0, base + 2 :, :] = jnp.zeros_like(pack_ref[e, 0, base + 2 :, :])
    for f in range(fields):
        lines = edge_lines(functools.partial(field_tile, f), levels, width)
        for e in range(4):
            pack_ref[e, 0, f * levels : (f + 1) * levels, :] = lines[e] * wet_lines[e]


def to_rows(flat_ref, out_ref, width, masked):
    lane = lanes_of(SUBLANES)
    for i in range(width):
        t, skip = divmod(i * width, LANES)
        row = turn(flat_ref[:, t * LANES : (t + 1) * LANES], -skip)
        if skip + width > LANES:
            rest = turn(flat_ref[:, (t + 1) * LANES : (t + 2) * LANES], -skip)
            row = jnp.where(lane < LANES - skip, row, rest)
        if masked:
            row = jnp.where(lane < width, row, 0.0)
        out_ref[i] = row


def prepare_kernel(width, thick_ref, field_ref, wet_ref, diag_ref, u_ref, v_ref, wet_rows_ref, diag_rows_ref, flat_ref):
    _, _, levels, cells = field_ref.shape
    slot = pl.program_id(0)
    rows = rows_of(levels)
    weight = jnp.zeros((levels, LANES), F32)
    for l in range(levels):
        weight = jnp.where(rows == l, 0.5 * thick_ref[l], weight)

    @pl.when(slot == 0)
    def _():
        flat_ref[...] = jnp.zeros_like(flat_ref)

    for t in range(tile_count(cells)):
        keep = tile_lanes(cells, t)
        at = slice(t * LANES, t * LANES + keep)
        wet = wet_ref[0, :, at].astype(F32)
        factor = weight[:, :keep] * wet
        terms = (
            jnp.sum(field_ref[0, 0, :, at] * factor, axis=0, keepdims=True),
            jnp.sum(field_ref[0, 1, :, at] * factor, axis=0, keepdims=True),
            wet,
            diag_ref[0, :, at],
        )
        mine = rows_of(SUBLANES)[:, :keep] == slot
        for n, term in enumerate(terms):
            flat_ref[n, :, at] = jnp.where(mine, term, flat_ref[n, :, at])

    @pl.when(slot == pl.num_programs(0) - 1)
    def _():
        to_rows(flat_ref.at[0], u_ref, width, False)
        to_rows(flat_ref.at[1], v_ref, width, False)
        to_rows(flat_ref.at[2], wet_rows_ref, width, True)
        to_rows(flat_ref.at[3], diag_rows_ref, width, False)


def strip_place(shift, strips):
    return jnp.bitwise_and(shift, 1) if strips == 2 else jnp.where(shift < 0, 2, shift)


def partner_block(links_ref, k, e, strips, slots, up_ref, down_ref, beside_ref):
    group_shift = links_ref[k, e, 0]
    place = strip_place(links_ref[k, e, 1], strips)
    entry = (e ^ 1) * slots + jnp.maximum(links_ref[k, e, 2], 0)
    far = place * (4 * slots) + entry
    if e == 0:
        return up_ref[far]
    if e == 1:
        return down_ref[far]
    near = jnp.maximum(place - 1, 0) * (4 * slots) + entry
    upper = (group_shift < 0).astype(F32)
    lower = (group_shift > 0).astype(F32)
    middle = 1.0 - upper - lower
    return upper * up_ref[far] + lower * down_ref[far] + middle * beside_ref[near]


def seam_numbers(links_ref, k, e):
    code = links_ref[k, e, 3]
    live = (links_ref[k, e, 2] >= 0).astype(F32)
    cosine = (code == 0).astype(F32) - (code == 2).astype(F32)
    sine = (code == 1).astype(F32) - (code == 3).astype(F32)
    return (code != 0).astype(jnp.int32), live, cosine, sine


def backward_step(lane, width):
    return jnp.where(lane < width, width - 1 - 2 * lane, 0)


def side_columns(lines_ref, width):
    lane = lanes_of(SUBLANES)
    west = lines_ref[0:SUBLANES, :]
    east = turn(lines_ref[SUBLANES : 2 * SUBLANES, :], width - 1)

    def column(i):
        return turn(jnp.where(lane == i, west, east), -i)

    return column


def source_kernel(width, strips, links_ref, thick_ref, up_ref, down_ref, beside_ref, u_ref, v_ref, wet_ref,
                  r_ref, pack_ref, rims_ref, wet_lines_ref, diag_lines_ref, normal_ref):
    slots = links_ref.shape[0]
    fields, levels = rims_ref.shape[1:3]
    depth = up_ref.shape[1]
    pair = 2 * levels
    base = fields * levels
    lane_all = lanes_of(depth)
    mirror = backward_step(lane_all, width)
    rows = rows_of(pair)
    sign = jnp.where(rows < levels, 1.0, -1.0)
    weight_u = jnp.zeros((pair, LANES), F32)
    weight_v = jnp.zeros((pair, LANES), F32)
    for l in range(levels):
        weight_u = jnp.where(rows == l, 0.5 * thick_ref[l], weight_u)
        weight_v = jnp.where(rows == levels + l, 0.5 * thick_ref[l], weight_v)
    normal_ref[...] = jnp.zeros_like(normal_ref)
    wet_lines_ref[...] = jnp.zeros_like(wet_lines_ref)
    diag_lines_ref[...] = jnp.zeros_like(diag_lines_ref)
    for e in range(4):
        for k in range(slots):
            flip, live, cosine, sine = seam_numbers(links_ref, k, e)
            block = partner_block(links_ref, k, e, strips, slots, up_ref, down_ref, beside_ref)
            block = take_lanes(block, lane_all + flip * mirror) * live
            both = block[:pair]
            turned = cosine * both + (sine * sign) * pltpu.roll(both, levels, 0)
            at = e * slots + k
            rims_ref[at, 0] = turned[:levels]
            rims_ref[at, 1] = turned[levels:pair]
            rims_ref[at, 2] = block[pair:base]
            line = slice(e * SUBLANES + k, e * SUBLANES + k + 1)
            wet_lines_ref[line, :] = block[base : base + 1]
            diag_lines_ref[line, :] = block[base + 1 : base + 2]
            normal_ref[line, :] = jnp.sum(turned * (weight_u if e < 2 else weight_v), axis=0, keepdims=True)
    lane = lanes_of(SUBLANES)
    column = side_columns(normal_ref, width)
    zero = jnp.zeros((SUBLANES, LANES), F32)
    lines = [[zero, zero], [zero, zero]]
    for i in range(width):
        across = u_ref[i]
        ends = column(i)
        west = jnp.where(lane == 0, ends, turn(across, 1))
        east = jnp.where(lane == width - 1, ends, turn(across, -1))
        south = v_ref[i - 1] if i > 0 else normal_ref[2 * SUBLANES : 3 * SUBLANES, :]
        north = v_ref[i + 1] if i < width - 1 else normal_ref[3 * SUBLANES : 4 * SUBLANES, :]
        row = wet_ref[i] * (east - west + north - south)
        r_ref[i] = row
        here = lane == i
        for e in range(2):
            for d in range(2):
                origin = d if e == 0 else width - 1 - d
                lines[e][d] = jnp.where(here, turn(row, i - origin), lines[e][d])
    lines.append([r_ref[0], r_ref[1]])
    lines.append([r_ref[width - 1], r_ref[width - 2]])
    for e in range(4):
        for k in range(slots):
            for d in range(2):
                pack_ref[e * slots + k, d : d + 1, :] = lines[e][d][k : k + 1]


def operator_rows(x_ref, lines_ref, diag_ref, wet_ref, out_ref, width):
    lane = lanes_of(SUBLANES)
    column = side_columns(lines_ref, width)
    for i in range(width):
        x = x_ref[i]
        ends = column(i)
        west = jnp.where(lane == 0, ends, turn(x, 1))
        east = jnp.where(lane == width - 1, ends, turn(x, -1))
        south = x_ref[i - 1] if i > 0 else lines_ref[2 * SUBLANES : 3 * SUBLANES, :]
        north = x_ref[i + 1] if i < width - 1 else lines_ref[3 * SUBLANES : 4 * SUBLANES, :]
        out_ref[i] = wet_ref[i] * ((4.0 + diag_ref[i]) * x - (west + east + south + north))


def dotted(a_ref, b_ref, width, chunk=10):
    total = None
    for start in range(0, width, chunk):
        part = None
        for i in range(start, min(start + chunk, width)):
            term = a_ref[i] * b_ref[i]
            part = term if part is None else part + term
        total = part if total is None else total + part
    return jnp.sum(total, axis=(0, 1), keepdims=True)


def apply_kernel(width, strips, links_ref, up_ref, down_ref, beside_ref, pack_ref, r_ref, wet_ref, diag_ref,
                 wet_lines_ref, diag_lines_ref, q_ref, w_ref, row_ref, first_ref, second_ref, own_ref, flip_ref, far_ref):
    slots = links_ref.shape[0]
    total = 4 * SUBLANES
    for ref in (first_ref, second_ref, own_ref):
        ref[...] = jnp.zeros_like(ref)
    flip_ref[...] = jnp.zeros_like(flip_ref)
    table = jnp.full((1, LANES), -1, jnp.int32)
    lane1 = lanes_of(1)
    places = 2 if strips == 2 else 3
    for e in range(4):
        for k in range(slots):
            flip, live, _, _ = seam_numbers(links_ref, k, e)
            block = partner_block(links_ref, k, e, strips, slots, up_ref, down_ref, beside_ref) * live
            line = slice(e * SUBLANES + k, e * SUBLANES + k + 1)
            first_ref[line, :] = block[0:1]
            second_ref[line, :] = block[1:2]
            own_ref[line, :] = pack_ref[e * slots + k, 0:1, :]
            flip_ref[line, :] = jnp.full((1, LANES), flip, jnp.int32)
            partner = links_ref[k, e, 2]
            near = (links_ref[k, e, 0] + 1) * places + strip_place(links_ref[k, e, 1], strips)
            for end in range(2):
                from_lane = partner * ENDS + (e ^ 1) * 2 + (end + flip - 2 * end * flip)
                entry = jnp.where(partner >= 0, near * 32 + from_lane, -1)
                table = jnp.where(lane1 == k * ENDS + e * 2 + end, entry, table)
    lane_all = lanes_of(total)
    index = lane_all + flip_ref[...] * backward_step(lane_all, width)
    first = take_lanes(first_ref[...], index)
    second = take_lanes(second_ref[...], index)
    first_ref[...] = first
    beside = second + own_ref[...] + turn(first, 1) + turn(first, -1)
    far_ref[...] = wet_lines_ref[...] * ((4.0 + diag_lines_ref[...]) * first - beside)

    operator_rows(r_ref, first_ref, diag_ref, wet_ref, q_ref, width)
    operator_rows(q_ref, far_ref, diag_ref, wet_ref, w_ref, width)

    lane = lanes_of(SUBLANES)
    block_of = rows_of(SUBLANES) == lane // ENDS
    which = lane % ENDS
    side = which // 2
    end = which % 2
    column = jnp.where(side < 2, side, end) * (width - 1)
    upper = jnp.where(side < 2, end, side - 2) == 1
    corner = jnp.where(upper, take_lanes(q_ref[width - 1], column), take_lanes(q_ref[0], column))
    corner = jnp.sum(jnp.where(block_of, corner, 0.0), axis=0, keepdims=True)
    seen = jnp.zeros((SUBLANES, LANES), F32)
    for e in range(4):
        ends = take_lanes(far_ref[e * SUBLANES : (e + 1) * SUBLANES, :], end * (width - 1))
        seen = jnp.where(block_of & (side == e), ends, seen)
    seen = jnp.sum(seen, axis=0, keepdims=True)
    row = jnp.where(lane1 < 32, corner, 0.0)
    row = jnp.where((lane1 >= 32) & (lane1 < 64), turn(seen, 32), row)
    row = jnp.where((lane1 >= 64) & (lane1 < 96), turn(table.astype(F32), 64), row)
    sums = (dotted(r_ref, r_ref, width), dotted(r_ref, q_ref, width), dotted(q_ref, q_ref, width), dotted(q_ref, w_ref, width))
    for n, value in enumerate(sums):
        row = jnp.where(lane1 == 96 + n, value, row)
    row_ref[...] = row


def finish_kernel(width, groups, strips, rows_ref, r_ref, q_ref, w_ref, wet_ref, x_ref, res_ref, sol_rows, res_rows):
    devices = groups * strips
    slots, _, cells = x_ref.shape
    table = rows_ref[...]
    lane = lanes_of(devices)
    row = rows_of(devices)
    me = lax.axis_index("tiles") * strips + lax.axis_index("strip")
    strip = row % strips
    link = jnp.where(lane < 32, turn(table, -64), -1.0).astype(jnp.int32)
    near = jnp.where(link < 0, -1, link // 32)
    from_lane = jnp.where(link < 0, 0, link % 32)

    def by_rows(value, shift):
        shift %= devices
        return value if shift == 0 else pltpu.roll(value, shift, 0)

    shifts = (0, 1) if strips == 2 else (0, 1, -1)
    exact = jnp.zeros_like(table)
    for group_shift in (-1, 0, 1):
        shifted = by_rows(table, -group_shift * strips)
        for place, strip_shift in enumerate(shifts):
            if group_shift == 0 and strip_shift == 0:
                continue
            if strip_shift == 0:
                there = shifted
            elif strip_shift == 1:
                there = jnp.where(strip < strips - 1, by_rows(shifted, -1), by_rows(shifted, strips - 1))
            else:
                there = jnp.where(strip > 0, by_rows(shifted, 1), by_rows(shifted, 1 - strips))
            taken = take_lanes(there, from_lane)
            exact = jnp.where(near == (group_shift + 1) * len(shifts) + place, taken, exact)
    change = jnp.where(near >= 0, turn(table, -32) - exact, 0.0)
    product = jnp.sum(table * change, axis=(0, 1), keepdims=True)
    sums = jnp.sum(table, axis=0, keepdims=True)
    lane1 = lanes_of(1)
    rr, rq, qq, qw = (jnp.sum(jnp.where(lane1 == 96 + n, sums, 0.0), axis=1, keepdims=True) for n in range(4))
    qw = qw + product
    alpha = rr / rq
    next_rr = rr - 2.0 * alpha * rq + alpha * alpha * qq
    image = rq - 2.0 * alpha * qq + alpha * alpha * qw
    ratio = next_rr / rr
    second = next_rr / (image - ratio * next_rr / alpha)

    mine = jnp.sum(jnp.where(row == me, change, 0.0), axis=0, keepdims=True)
    mine = jnp.broadcast_to(mine, (SUBLANES, LANES))
    lane8 = lanes_of(SUBLANES)
    slot8 = rows_of(SUBLANES) * ENDS

    def both(a, b):
        return take_lanes(mine, slot8 + a) + take_lanes(mine, slot8 + b)

    def ends(west, east):
        return jnp.where(lane8 == 0, west, jnp.where(lane8 == width - 1, east, 0.0))

    for i in range(width):
        r = r_ref[i]
        q = q_ref[i]
        w = w_ref[i]
        if i == 0:
            w = w + wet_ref[i] * ends(both(0, 4), both(2, 5))
        elif i == width - 1:
            w = w + wet_ref[i] * ends(both(1, 6), both(3, 7))
        residual = r - alpha * q
        direction = residual + ratio * r
        sol_rows[i] = alpha * r + second * direction
        res_rows[i] = residual - second * (q - alpha * w + ratio * q)
    for rows_from, out_ref in ((sol_rows, x_ref), (res_rows, res_ref)):
        for t in range(tile_count(cells)):
            keep = tile_lanes(cells, t)
            value = None
            for i in range(t * LANES // width, (t * LANES + keep - 1) // width + 1):
                start = i * width - t * LANES
                piece = turn(rows_from[i], start)
                value = piece if value is None else jnp.where(lane8 >= start, piece, value)
            for k in range(slots):
                out_ref[k, :, t * LANES : t * LANES + keep] = value[k : k + 1, :keep]


def slab_kernel(width, spread_ref, mixing_ref, field_ref, wet_ref, rims_ref, out_ref, masked_ref):
    _, fields, levels, cells = field_ref.shape
    tiles = tile_count(cells)
    lane = lanes_of(levels)
    rows = rows_of(levels)
    wrap = LANES - width
    start = cells - width

    def one_field(f, carry):
        spread = jnp.zeros((levels, LANES), F32)
        mixing = jnp.zeros((levels, LANES), F32)
        for l in range(levels):
            spread = jnp.where(rows == l, spread_ref[f, l], spread)
            mixing = jnp.where(rows == l, mixing_ref[l], mixing)
        masked_ref[:, (tiles - 1) * LANES :] = jnp.zeros((levels, LANES), F32)
        for t in range(tiles):
            at = slice(t * LANES, t * LANES + tile_lanes(cells, t))
            masked_ref[:, at] = field_ref[0, f, :, at] * wet_ref[0, :, at].astype(F32)
        west_rim, east_rim, south_rim, north_rim = (rims_ref[e, 0, f] for e in range(4))
        north_rim = turn(north_rim, start)

        def tile(t):
            return masked_ref[:, t * LANES : (t + 1) * LANES]

        for t in range(tiles):
            keep = tile_lanes(cells, t)
            at = slice(t * LANES, t * LANES + keep)
            value = tile(t)
            before = tile(t - 1) if t > 0 else value
            after = tile(t + 1) if t < tiles - 1 else value
            west = jnp.where(lane == 0, turn(before, 1), turn(value, 1))
            east = jnp.where(lane == LANES - 1, turn(after, -1), turn(value, -1))
            south = jnp.where(lane < width, turn(before, width), turn(value, width))
            north = jnp.where(lane < wrap, turn(value, -width), turn(after, -width))
            for b, place, is_west, is_east in seams(width, t):
                rim = turn(jnp.where(lane < b, east_rim, west_rim), place - b)
                if is_west:
                    west = jnp.where(lane == place % LANES, rim, west)
                if is_east:
                    east = jnp.where(lane == (place - 1) % LANES, rim, east)
            if t * LANES < width:
                south = jnp.where(lane < width, south_rim, south)
            if (t + 1) * LANES > start:
                north = jnp.where(lane >= start - t * LANES, north_rim, north)
            flat = west + east + south + north - 4.0 * value
            above = jnp.concatenate([value[1:], value[levels - 1 :]], axis=0)
            below = jnp.concatenate([value[:1], value[: levels - 1]], axis=0)
            column = above + below - 2.0 * value
            updated = value + spread * flat + mixing * column
            out_ref[0, f, :, at] = wet_ref[0, :, at].astype(F32) * updated[:, :keep]
        return carry

    lax.fori_loop(0, fields, one_field, 0)


def cost(flops, moved):
    return pl.CostEstimate(flops=flops, bytes_accessed=moved, transcendentals=0)


def exchange(pack, groups, strips):
    def along(value, axis, size, step):
        return lax.ppermute(value, axis, [(i, (i + step) % size) for i in range(size)])

    beside = along(pack, "strip", strips, -1)
    if strips > 2:
        beside = jnp.concatenate([beside, along(pack, "strip", strips, 1)], axis=0)
    stack = jnp.concatenate([pack, beside], axis=0)
    return along(stack, "tiles", groups, 1), along(stack, "tiles", groups, -1), beside


def on_device(groups, strips, fields, wet_land, links, surface_diagonal, spread, mixing, thickness):
    field = fields[0, 0]
    slots, kinds, levels, cells = field.shape
    width = math.isqrt(cells)
    wet = wet_land.reshape(slots, 1, cells)
    diag = surface_diagonal.reshape(slots, 1, cells)
    seam = links[0, 0]
    depth = -(-(kinds * levels + 2) // SUBLANES) * SUBLANES
    bulk = 4 * field.size
    sides = 4 * slots

    def shape(*dims):
        return jax.ShapeDtypeStruct(dims, F32)

    def per_slot(count):
        return pl.BlockSpec((1, count, levels, cells), lambda s: (s, 0, 0, 0))

    line = pl.BlockSpec((1, 1, cells), lambda s: (s, 0, 0))
    rows = shape(width, SUBLANES, LANES)
    whole_rows = pl.BlockSpec((width, SUBLANES, LANES), lambda s: (0, 0, 0))
    lines = shape(4 * SUBLANES, LANES)
    lines_scratch = pltpu.VMEM((4 * SUBLANES, LANES), F32)

    pack = pl.pallas_call(
        functools.partial(pack_kernel, width),
        grid=(slots,),
        in_specs=[per_slot(kinds), line, line],
        out_specs=pl.BlockSpec((4, 1, depth, LANES), lambda s: (0, s, 0, 0)),
        out_shape=shape(4, slots, depth, LANES),
        scratch_shapes=[pltpu.VMEM((depth, LANES), F32)],
        cost_estimate=cost(bulk, bulk),
        name="pack_rims",
    )(field, wet, diag).reshape(sides, depth, LANES)
    up, down, beside = exchange(pack, groups, strips)

    u, v, wet_rows, diag_rows = pl.pallas_call(
        functools.partial(prepare_kernel, width),
        grid=(slots,),
        in_specs=[SMEM, per_slot(2), line, line],
        out_specs=[whole_rows] * 4,
        out_shape=[rows] * 4,
        scratch_shapes=[pltpu.VMEM((4, SUBLANES, tile_count(cells) * LANES), F32)],
        cost_estimate=cost(64 * bulk, bulk),
        name="prepare_rows",
    )(thickness, field, wet, diag)

    r, pack2, rims, wet_lines, diag_lines = pl.pallas_call(
        functools.partial(source_kernel, width, strips),
        in_specs=[SMEM, SMEM] + [VMEM] * 6,
        out_specs=[VMEM] * 5,
        out_shape=[rows, shape(sides, 2, LANES), shape(sides, kinds, levels, LANES), lines, lines],
        scratch_shapes=[lines_scratch],
        cost_estimate=cost(bulk, bulk),
        name="source_rows",
    )(seam, thickness, up, down, beside, u, v, wet_rows)
    up, down, beside = exchange(pack2, groups, strips)

    updated = pl.pallas_call(
        functools.partial(slab_kernel, width),
        grid=(slots,),
        in_specs=[SMEM, SMEM, per_slot(kinds), line,
                  pl.BlockSpec((4, 1, kinds, levels, LANES), lambda s: (0, s, 0, 0, 0))],
        out_specs=per_slot(kinds),
        out_shape=shape(slots, kinds, levels, cells),
        scratch_shapes=[pltpu.VMEM((levels, tile_count(cells) * LANES), F32)],
        cost_estimate=cost(64 * bulk, 2 * bulk),
        name="slab_step",
    )(spread, mixing, field, wet, rims.reshape(4, slots, kinds, levels, LANES))

    q, w, row = pl.pallas_call(
        functools.partial(apply_kernel, width, strips),
        in_specs=[SMEM] + [VMEM] * 9,
        out_specs=[VMEM] * 3,
        out_shape=[rows, rows, shape(1, LANES)],
        scratch_shapes=[lines_scratch] * 3 + [pltpu.VMEM((4 * SUBLANES, LANES), jnp.int32), lines_scratch],
        cost_estimate=cost(bulk, bulk),
        name="apply_twice",
    )(seam, up, down, beside, pack2, r, wet_rows, diag_rows, wet_lines, diag_lines)

    spread_rows = jnp.broadcast_to(row[None], (groups * strips, 1, LANES))
    table = lax.all_to_all(spread_rows, ("tiles", "strip"), 0, 0).reshape(groups * strips, LANES)

    surface = shape(slots, 1, cells)
    x, res = pl.pallas_call(
        functools.partial(finish_kernel, width, groups, strips),
        in_specs=[VMEM] * 5,
        out_specs=[VMEM] * 2,
        out_shape=[surface, surface],
        scratch_shapes=[pltpu.VMEM((width, SUBLANES, LANES), F32)] * 2,
        cost_estimate=cost(bulk, bulk),
        name="finish",
    )(table, r, q, w, wet_rows)
    return updated[None, None], x.reshape(1, 1, slots, cells), res.reshape(1, 1, slots, cells)


def solution(mesh):
    wide = P("tiles", "strip", None, None, None, None)
    flat = P("tiles", "strip", None, None)
    return jax.shard_map(
        functools.partial(on_device, mesh.shape["tiles"], mesh.shape["strip"]),
        mesh=mesh,
        in_specs=(wide, flat, P("tiles", "strip", None, None, None), flat, P(), P(), P()),
        out_specs=(wide, flat, flat),
        check_vma=False,
    )
```

```python
import functools
import math

import jax
import jax.numpy as jnp
from jax import lax
from jax.experimental import pallas as pl
from jax.experimental.pallas import tpu as pltpu
from jax.sharding import PartitionSpec as P

LANES = 128
SUBLANES = 8
ENDS = 8
F32 = jnp.float32
VMEM = pl.BlockSpec(memory_space=pltpu.VMEM)
SMEM = pl.BlockSpec(memory_space=pltpu.SMEM)


def lanes_of(rows):
    return lax.broadcasted_iota(jnp.int32, (rows, LANES), 1)


def rows_of(rows):
    return lax.broadcasted_iota(jnp.int32, (rows, LANES), 0)


def turn(value, shift):
    shift %= LANES
    return value if shift == 0 else pltpu.roll(value, shift, 1)


def take_lanes(value, index):
    return jnp.take_along_axis(value, index, axis=1, mode="promise_in_bounds")


def tile_count(cells):
    return -(-cells // LANES)


def tile_lanes(cells, tile):
    return min(LANES, cells - tile * LANES)


def seams(width, tile):
    found = []
    for b in range(width + 1):
        place = b * width
        west = b < width and place // LANES == tile
        east = b > 0 and (place - 1) // LANES == tile
        if west or east:
            found.append((b, place, west, east))
    return found


def side_lines(tile_of, rows, width, depth):
    cells = width * width
    lane = lanes_of(rows)
    zero = jnp.zeros((rows, LANES), F32)
    classes = 2 * depth
    kept = [zero] * classes
    for t in range(tile_count(cells)):
        for b in range(width + 1):
            place = b * width
            near = [
                o
                for o in range(-depth if b > 0 else 0, depth if b < width else 0)
                if (place + o) // LANES == t
            ]
            if near:
                inside = ((lane - (b + near[0])) & (LANES - 1)) < len(near)
                kept[b % classes] = jnp.where(inside, turn(tile_of(t), b - place), kept[b % classes])

    def straight(start):
        t, skip = divmod(start, LANES)
        value = turn(tile_of(t), -skip)
        if skip + width > LANES:
            value = jnp.where(lane < LANES - skip, value, turn(tile_of(t + 1), -skip))
        return jnp.where(lane < width, value, 0.0)

    west, east = [], []
    for d in range(depth):
        w, e = zero, zero
        for c in range(classes):
            w = jnp.where(lane % classes == c, turn(kept[c], -d), w)
            e = jnp.where((lane + 1) % classes == c, turn(kept[c], d), e)
        west.append(jnp.where(lane < width, w, 0.0))
        east.append(jnp.where(lane < width, e, 0.0))
    south = [straight(d * width) for d in range(depth)]
    north = [straight(cells - (d + 1) * width) for d in range(depth)]
    return west, east, south, north


def pack_kernel(width, thick_ref, field_hbm, wet_hbm, diag_hbm, pack_ref, field_ref, wet_ref, diag_ref, tail_ref, sems):
    slots, fields, levels, cells = field_hbm.shape
    copies = [pltpu.make_async_copy(wet_hbm, wet_ref, sems.at[0]), pltpu.make_async_copy(diag_hbm, diag_ref, sems.at[1])]
    copies += [pltpu.make_async_copy(field_hbm.at[k], field_ref.at[k], sems.at[2 + k]) for k in range(slots)]
    for copy in copies:
        copy.start()
    copies[0].wait()
    copies[1].wait()
    last = tile_count(cells) - 1
    keep = tile_lanes(cells, last)
    tail_ref[...] = jnp.zeros_like(tail_ref)
    base = fields * levels
    rows = rows_of(levels)
    weight = jnp.zeros((levels, LANES), F32)
    for l in range(levels):
        weight = jnp.where(rows == l, 0.5 * thick_ref[l], weight)
    for k in range(slots):
        copies[2 + k].wait()
        for f in range(fields):
            tail_ref[k, f * levels : (f + 1) * levels, :keep] = field_ref[k, f, :, last * LANES : cells]
        tail_ref[k, base : base + 1, :keep] = wet_ref[k, :, last * LANES : cells].astype(F32)
        tail_ref[k, base + 1 : base + 2, :keep] = diag_ref[k, :, last * LANES : cells]

        def field_tile(f, t):
            if t == last:
                return tail_ref[k, f * levels : (f + 1) * levels, :]
            return field_ref[k, f, :, t * LANES : (t + 1) * LANES]

        def wet_tile(t):
            if t == last:
                return tail_ref[k, base : base + 1, :]
            return wet_ref[k, :, t * LANES : (t + 1) * LANES].astype(F32)

        def diag_tile(t):
            if t == last:
                return tail_ref[k, base + 1 : base + 2, :]
            return diag_ref[k, :, t * LANES : (t + 1) * LANES]

        wet = side_lines(wet_tile, 1, width, 3)
        diag = side_lines(diag_tile, 1, width, 1)
        parts = [side_lines(functools.partial(field_tile, f), levels, width, 3 if f < 2 else 1) for f in range(fields)]
        for e in range(4):
            at = e * slots + k
            for f in range(fields):
                pack_ref[at, f * levels : (f + 1) * levels, :] = parts[f][e][0] * wet[e][0]

            def weighted(f, d):
                return jnp.sum(parts[f][e][d] * weight * wet[e][d], axis=0, keepdims=True)

            normal, along = (0, 1) if e < 2 else (1, 0)
            extra = (wet[e][0], diag[e][0], wet[e][1], weighted(normal, 1), weighted(normal, 2), weighted(along, 1))
            for n, value in enumerate(extra):
                pack_ref[at, base + n : base + n + 1, :] = value
            pack_ref[at, base + len(extra) :, :] = jnp.zeros((pack_ref.shape[1] - base - len(extra), LANES), F32)


def to_rows(flat_ref, out_ref, width, masked):
    lane = lanes_of(SUBLANES)
    for i in range(width):
        t, skip = divmod(i * width, LANES)
        row = turn(flat_ref[:, t * LANES : (t + 1) * LANES], -skip)
        if skip + width > LANES:
            rest = turn(flat_ref[:, (t + 1) * LANES : (t + 2) * LANES], -skip)
            row = jnp.where(lane < LANES - skip, row, rest)
        if masked:
            row = jnp.where(lane < width, row, 0.0)
        out_ref[i] = row


def prepare_kernel(width, thick_ref, field_ref, wet_ref, diag_ref, u_ref, v_ref, wet_rows_ref, diag_rows_ref, flat_ref):
    _, _, levels, cells = field_ref.shape
    slot = pl.program_id(0)
    rows = rows_of(levels)
    weight = jnp.zeros((levels, LANES), F32)
    for l in range(levels):
        weight = jnp.where(rows == l, 0.5 * thick_ref[l], weight)

    @pl.when(slot == 0)
    def _():
        flat_ref[...] = jnp.zeros_like(flat_ref)

    for t in range(tile_count(cells)):
        keep = tile_lanes(cells, t)
        at = slice(t * LANES, t * LANES + keep)
        wet = wet_ref[0, :, at].astype(F32)
        factor = weight[:, :keep] * wet
        terms = (
            jnp.sum(field_ref[0, 0, :, at] * factor, axis=0, keepdims=True),
            jnp.sum(field_ref[0, 1, :, at] * factor, axis=0, keepdims=True),
            wet,
            diag_ref[0, :, at],
        )
        mine = rows_of(SUBLANES)[:, :keep] == slot
        for n, term in enumerate(terms):
            flat_ref[n, :, at] = jnp.where(mine, term, flat_ref[n, :, at])

    @pl.when(slot == pl.num_programs(0) - 1)
    def _():
        to_rows(flat_ref.at[0], u_ref, width, False)
        to_rows(flat_ref.at[1], v_ref, width, False)
        to_rows(flat_ref.at[2], wet_rows_ref, width, True)
        to_rows(flat_ref.at[3], diag_rows_ref, width, False)


def strip_place(shift, strips):
    return jnp.bitwise_and(shift, 1) if strips == 2 else jnp.where(shift < 0, 2, shift)


def partner_block(links_ref, k, e, strips, slots, up_ref, down_ref, beside_ref):
    group_shift = links_ref[k, e, 0]
    place = strip_place(links_ref[k, e, 1], strips)
    entry = (e ^ 1) * slots + jnp.maximum(links_ref[k, e, 2], 0)
    far = place * (4 * slots) + entry
    if e == 0:
        return up_ref[far]
    if e == 1:
        return down_ref[far]
    near = jnp.maximum(place - 1, 0) * (4 * slots) + entry
    upper = (group_shift < 0).astype(F32)
    lower = (group_shift > 0).astype(F32)
    middle = 1.0 - upper - lower
    return upper * up_ref[far] + lower * down_ref[far] + middle * beside_ref[near]


def seam_numbers(links_ref, k, e):
    code = links_ref[k, e, 3]
    live = (links_ref[k, e, 2] >= 0).astype(F32)
    cosine = (code == 0).astype(F32) - (code == 2).astype(F32)
    sine = (code == 1).astype(F32) - (code == 3).astype(F32)
    return (code != 0).astype(jnp.int32), live, cosine, sine


def backward_step(lane, width):
    return jnp.where(lane < width, width - 1 - 2 * lane, 0)


def side_columns(lines_ref, width):
    lane = lanes_of(SUBLANES)
    west = lines_ref[0:SUBLANES, :]
    east = turn(lines_ref[SUBLANES : 2 * SUBLANES, :], width - 1)

    def column(i):
        return turn(jnp.where(lane == i, west, east), -i)

    return column


def operator_rows(x_ref, lines_ref, diag_ref, wet_ref, out_ref, width):
    lane = lanes_of(SUBLANES)
    column = side_columns(lines_ref, width)
    for i in range(width):
        x = x_ref[i]
        ends = column(i)
        west = jnp.where(lane == 0, ends, turn(x, 1))
        east = jnp.where(lane == width - 1, ends, turn(x, -1))
        south = x_ref[i - 1] if i > 0 else lines_ref[2 * SUBLANES : 3 * SUBLANES, :]
        north = x_ref[i + 1] if i < width - 1 else lines_ref[3 * SUBLANES : 4 * SUBLANES, :]
        out_ref[i] = wet_ref[i] * ((4.0 + diag_ref[i]) * x - (west + east + south + north))


def dotted(a_ref, b_ref, width, chunk=10):
    total = None
    for start in range(0, width, chunk):
        part = None
        for i in range(start, min(start + chunk, width)):
            term = a_ref[i] * b_ref[i]
            part = term if part is None else part + term
        total = part if total is None else total + part
    return jnp.sum(total, axis=(0, 1), keepdims=True)


def lines_kernel(width, strips, links_ref, thick_ref, up_ref, down_ref, beside_ref, own_ref,
                 rims_ref, kept_ref, table_ref, lines_ref, numbers_ref):
    slots = links_ref.shape[0]
    fields, levels = rims_ref.shape[1:3]
    depth = up_ref.shape[1]
    pair = 2 * levels
    base = fields * levels
    stride = slots * ENDS
    lane_all = lanes_of(depth)
    mirror = backward_step(lane_all, width)
    rows = rows_of(pair)
    sign = jnp.where(rows < levels, 1.0, -1.0)
    weights = []
    for start in (0, levels):
        weight = jnp.zeros((pair, LANES), F32)
        for l in range(levels):
            weight = jnp.where(rows == start + l, 0.5 * thick_ref[l], weight)
        weights.append(weight)
    places = 2 if strips == 2 else 3
    lane1 = lanes_of(1)
    lines_ref[...] = jnp.zeros_like(lines_ref)
    numbers_ref[...] = jnp.zeros_like(numbers_ref)
    code_ref = table_ref
    table = jnp.full((1, LANES), -1, jnp.int32)
    ends = [(e, k) for e in range(4) for k in range(slots)]
    numbers = {at: seam_numbers(links_ref, at[1], at[0]) for at in ends}
    blocks = {at: partner_block(links_ref, at[1], at[0], strips, slots, up_ref, down_ref, beside_ref) for at in ends}
    for at in ends:
        flip, live, _, _ = numbers[at]
        blocks[at] = take_lanes(blocks[at], lane_all + flip * mirror) * live

    def summed(value, weight):
        return jnp.sum(value * weight, axis=0, keepdims=True)

    for at in ends:
        e, k = at
        flip, live, cosine, sine = numbers[at]
        block = blocks[at]
        both = block[:pair]
        turned = cosine * both + (sine * sign) * pltpu.roll(both, levels, 0)
        side = e * slots + k
        rims_ref[side, 0] = turned[:levels]
        rims_ref[side, 1] = turned[levels:pair]
        rims_ref[side, 2] = block[pair:base]
        line = slice(e * SUBLANES + k, e * SUBLANES + k + 1)
        for n in range(6):
            lines_ref[n, line, :] = block[base + n : base + n + 1]
        normal, along = weights if e < 2 else weights[::-1]
        mine = own_ref[side, :pair, :]
        lines_ref[6, line, :] = summed(both, normal)
        lines_ref[7, line, :] = summed(both, along)
        lines_ref[8, line, :] = summed(mine, normal)
        lines_ref[9, line, :] = summed(mine, along)
        lines_ref[10, line, :] = own_ref[side, base : base + 1, :]
        lines_ref[11, line, :] = own_ref[side, base + 3 : base + 4, :]
        numbers_ref[0, line, :] = jnp.full((1, LANES), cosine, F32)
        numbers_ref[1, line, :] = jnp.full((1, LANES), sine if e < 2 else -sine, F32)
        numbers_ref[2, line, :] = jnp.full((1, LANES), 1.0 - 2.0 * flip.astype(F32), F32)
        partner = links_ref[k, e, 2]
        near = (links_ref[k, e, 0] + 1) * places + strip_place(links_ref[k, e, 1], strips)
        for end in range(2):
            from_lane = partner * ENDS + (e ^ 1) * 2 + (end + flip - 2 * end * flip)
            entry = jnp.where(partner >= 0, near * 32 + from_lane, -1)
            table = jnp.where(lane1 == k * ENDS + e * 2 + end, entry, table)

    (wet1, diag1, wet2, normal2, normal3, along2, normal1, along1, normal0, along0, wet0, inner0) = (lines_ref[n] for n in range(12))
    cosine, sine, forward = (numbers_ref[n] for n in range(3))
    received = cosine * normal1 + sine * along1
    given = cosine * normal0 - sine * along0
    outward = jnp.where((rows_of(4 * SUBLANES) // SUBLANES) % 2 == 0, 1.0, -1.0)

    def slope(value):
        return turn(value, -1) - turn(value, 1)

    first = wet1 * (outward * (given - normal2) + forward * slope(along1))
    second = wet2 * (outward * (normal1 - normal3) + forward * slope(along2))
    lane8 = lanes_of(SUBLANES)

    def at_ends(e):
        low, high = (2, 3) if e < 2 else (0, 1)
        place = jnp.full((SUBLANES, LANES), (e % 2) * (width - 1), jnp.int32)
        before = take_lanes(received[low * SUBLANES : (low + 1) * SUBLANES], place)
        after = take_lanes(received[high * SUBLANES : (high + 1) * SUBLANES], place)
        return jnp.where(lane8 == 0, -before, jnp.where(lane8 == width - 1, after, 0.0))

    lateral = jnp.concatenate([at_ends(e) for e in range(4)], axis=0)
    own = wet0 * (outward * (inner0 - received) + slope(along0) + lateral)
    beside = second + own + turn(first, 1) + turn(first, -1)
    far = wet1 * ((4.0 + diag1) * first - beside)
    for n, value in enumerate((received, first, far, wet1)):
        kept_ref[n] = value
    code_ref[...] = table


def source_kernel(width, kept_ref, u_ref, v_ref, wet_ref, r_ref):
    lane = lanes_of(SUBLANES)
    column = side_columns(kept_ref.at[0], width)
    for i in range(width):
        across = u_ref[i]
        cells = column(i)
        west = jnp.where(lane == 0, cells, turn(across, 1))
        east = jnp.where(lane == width - 1, cells, turn(across, -1))
        south = v_ref[i - 1] if i > 0 else kept_ref[0, 2 * SUBLANES : 3 * SUBLANES, :]
        north = v_ref[i + 1] if i < width - 1 else kept_ref[0, 3 * SUBLANES : 4 * SUBLANES, :]
        r_ref[i] = wet_ref[i] * (east - west + north - south)


def operator_kernel(width, line, x_ref, kept_ref, diag_ref, wet_ref, out_ref):
    operator_rows(x_ref, kept_ref.at[line], diag_ref, wet_ref, out_ref, width)


def totals_kernel(width, slots, kept_ref, table_ref, r_ref, q_ref, w_ref, wet_ref, diag_ref, rows_ref, near_ref):
    stride = slots * ENDS
    lane1 = lanes_of(1)
    lane = lanes_of(SUBLANES)
    first, far, wet1 = kept_ref[1], kept_ref[2], kept_ref[3]
    table = table_ref[...]
    block_of = rows_of(SUBLANES) == lane // ENDS
    which = lane % ENDS
    side = which // 2
    end = which % 2
    upright = side < 2
    column = jnp.where(upright, side, end) * (width - 1)
    upper = jnp.where(upright, end, side - 2) == 1
    step = 1 + end * (width - 3)
    beside_column = jnp.where(upright, column, step)

    def in_row(value):
        value = jnp.sum(jnp.where(block_of, value, 0.0), axis=0, keepdims=True)
        return jnp.where(lane1 < stride, value, 0.0)

    def corners(ref):
        return in_row(jnp.where(upper, take_lanes(ref[width - 1], column), take_lanes(ref[0], column)))

    def of_lines(value, index):
        total = jnp.zeros((SUBLANES, LANES), F32)
        for e in range(4):
            total = jnp.where(side == e, take_lanes(value[e * SUBLANES : (e + 1) * SUBLANES], index), total)
        return in_row(total)

    lower_row = jnp.where(upright, take_lanes(q_ref[1], beside_column), take_lanes(q_ref[0], beside_column))
    upper_row = jnp.where(upright, take_lanes(q_ref[width - 2], beside_column), take_lanes(q_ref[width - 1], beside_column))
    q_next = in_row(jnp.where(upper, upper_row, lower_row))
    q_corner = corners(q_ref)
    near = of_lines(wet1, step)
    near_ref[...] = near
    sums = (dotted(r_ref, r_ref, width), dotted(r_ref, q_ref, width), dotted(q_ref, q_ref, width), dotted(q_ref, w_ref, width))
    total = jnp.zeros((1, LANES), F32)
    for n, value in enumerate(sums):
        total = jnp.where(lane1 == n, value, total)
    last = end * (width - 1)
    code = jnp.where(lane1 < stride, table, 0).astype(F32)
    diag_corner = corners(diag_ref)
    for n, values in enumerate((
        (corners(r_ref), of_lines(first, last), q_corner, of_lines(far, last), code),
        (corners(wet_ref), q_next * near - corners(w_ref), q_next, 4.0 + diag_corner, total),
    )):
        row = jnp.zeros((1, LANES), F32)
        for m, value in enumerate(values):
            row = jnp.where((lane1 >= m * stride) & (lane1 < (m + 1) * stride), turn(value, m * stride), row)
        rows_ref[:, n : n + 1, :] = jnp.broadcast_to(row[None], (rows_ref.shape[0], 1, LANES))


def finish_kernel(width, groups, strips, tables_ref, near_ref, r_ref, q_ref, w_ref, wet_ref, x_ref, res_ref, sol_rows, res_rows):
    devices = groups * strips
    slots, _, cells = x_ref.shape
    stride = slots * ENDS
    lane = lanes_of(devices)
    row = rows_of(devices)
    me = lax.axis_index("tiles") * strips + lax.axis_index("strip")
    strip = row % strips
    tables = [tables_ref[pl.ds(n, devices, stride=2), :] for n in range(2)]
    listed = lane < stride

    def part(n, m):
        return jnp.where(listed, turn(tables[n], -m * stride), 0.0)

    r_corner, first_seen, q_seen, far_seen, code = (part(0, m) for m in range(5))
    wet_corner, mixed, q_next, diag_corner, totals = (part(1, m) for m in range(5))
    link = jnp.where(listed, code, -1.0).astype(jnp.int32)
    near = jnp.where(link < 0, -1, link // 32)
    from_lane = jnp.where(link < 0, 0, link % 32)

    def by_rows(value, shift):
        shift %= devices
        return value if shift == 0 else pltpu.roll(value, shift, 0)

    shifts = (0, 1) if strips == 2 else (0, 1, -1)

    def from_partner(value):
        found = jnp.zeros_like(value)
        for group_shift in (-1, 0, 1):
            shifted = by_rows(value, -group_shift * strips)
            for place, strip_shift in enumerate(shifts):
                if group_shift == 0 and strip_shift == 0:
                    continue
                if strip_shift == 0:
                    there = shifted
                elif strip_shift == 1:
                    there = jnp.where(strip < strips - 1, by_rows(shifted, -1), by_rows(shifted, strips - 1))
                else:
                    there = jnp.where(strip > 0, by_rows(shifted, 1), by_rows(shifted, 1 - strips))
                taken = take_lanes(there, from_lane)
                found = jnp.where(near == (group_shift + 1) * len(shifts) + place, taken, found)
        return found

    rise = jnp.where(near >= 0, from_partner(r_corner) - first_seen, 0.0)
    which = lane % ENDS
    other = lane - which + (1 - which // 4) * 4 + (which % 2) * 2 + (which // 2) % 2
    at_corner = rise + take_lanes(rise, other)
    change = -wet_corner * at_corner
    q_corner = q_seen + change
    excess = jnp.where(near >= 0, from_partner(q_corner) - far_seen, 0.0)

    def overall(value):
        return jnp.sum(value, axis=(0, 1), keepdims=True)

    sums = jnp.sum(totals, axis=0, keepdims=True)
    lane1 = lanes_of(1)
    rr, rq, qq, qw = (jnp.sum(jnp.where(lane1 == n, sums, 0.0), axis=1, keepdims=True) for n in range(4))
    rq = rq - overall(r_corner * rise)
    qq = qq + overall(0.5 * wet_corner * at_corner * at_corner - 2.0 * q_seen * rise)
    qw = qw + overall(rise * mixed + q_corner * (0.5 * diag_corner * change - excess) - q_next * change)
    alpha = rr / rq
    next_rr = rr - 2.0 * alpha * rq + alpha * alpha * qq
    image = rq - 2.0 * alpha * qq + alpha * alpha * qw
    ratio = next_rr / rr
    second = next_rr / (image - ratio * next_rr / alpha)

    lane8 = lanes_of(SUBLANES)
    slot8 = rows_of(SUBLANES) * ENDS

    def own(value):
        value = jnp.sum(jnp.where(row == me, value, 0.0), axis=0, keepdims=True)
        return jnp.broadcast_to(value, (SUBLANES, LANES))

    own_change = own(change)
    at_corners = own(0.5 * diag_corner * change - excess)
    at_next = jnp.broadcast_to(near_ref[...], (SUBLANES, LANES)) * own(rise) - own_change

    def entry(value, n):
        return take_lanes(value, slot8 + n)

    def placed(values):
        total = jnp.zeros((SUBLANES, LANES), F32)
        for at, value in values:
            total = jnp.where(lane8 == at, value, total)
        return total

    w_change = {
        0: ((0, entry(at_corners, 0) + entry(at_corners, 4)), (width - 1, entry(at_corners, 2) + entry(at_corners, 5)),
            (1, entry(at_next, 4)), (width - 2, entry(at_next, 5))),
        1: ((0, entry(at_next, 0)), (width - 1, entry(at_next, 2))),
        width - 2: ((0, entry(at_next, 1)), (width - 1, entry(at_next, 3))),
        width - 1: ((0, entry(at_corners, 1) + entry(at_corners, 6)), (width - 1, entry(at_corners, 3) + entry(at_corners, 7)),
                    (1, entry(at_next, 6)), (width - 2, entry(at_next, 7))),
    }
    q_change = {
        0: ((0, entry(own_change, 0)), (width - 1, entry(own_change, 2))),
        width - 1: ((0, entry(own_change, 1)), (width - 1, entry(own_change, 3))),
    }
    for i in range(width):
        r = r_ref[i]
        q = q_ref[i]
        w = w_ref[i]
        if i in q_change:
            q = q + placed(q_change[i])
        if i in w_change:
            w = w + wet_ref[i] * placed(w_change[i])
        residual = r - alpha * q
        direction = residual + ratio * r
        sol_rows[i] = alpha * r + second * direction
        res_rows[i] = residual - second * (q - alpha * w + ratio * q)
    for rows_from, out_ref in ((sol_rows, x_ref), (res_rows, res_ref)):
        for t in range(tile_count(cells)):
            keep = tile_lanes(cells, t)
            value = None
            for i in range(t * LANES // width, (t * LANES + keep - 1) // width + 1):
                start = i * width - t * LANES
                piece = turn(rows_from[i], start)
                value = piece if value is None else jnp.where(lane8 >= start, piece, value)
            for k in range(slots):
                out_ref[k, :, t * LANES : t * LANES + keep] = value[k : k + 1, :keep]


def slab_kernel(width, spread_ref, mixing_ref, field_ref, wet_ref, rims_ref, out_ref, masked_ref):
    _, fields, levels, cells = field_ref.shape
    tiles = tile_count(cells)
    lane = lanes_of(levels)
    rows = rows_of(levels)
    wrap = LANES - width
    start = cells - width

    def one_field(f, carry):
        spread = jnp.zeros((levels, LANES), F32)
        mixing = jnp.zeros((levels, LANES), F32)
        for l in range(levels):
            spread = jnp.where(rows == l, spread_ref[f, l], spread)
            mixing = jnp.where(rows == l, mixing_ref[l], mixing)
        masked_ref[:, (tiles - 1) * LANES :] = jnp.zeros((levels, LANES), F32)
        for t in range(tiles):
            at = slice(t * LANES, t * LANES + tile_lanes(cells, t))
            masked_ref[:, at] = field_ref[0, f, :, at] * wet_ref[0, :, at].astype(F32)
        west_rim, east_rim, south_rim, north_rim = (rims_ref[e, 0, f] for e in range(4))
        north_rim = turn(north_rim, start)

        def tile(t):
            return masked_ref[:, t * LANES : (t + 1) * LANES]

        for t in range(tiles):
            keep = tile_lanes(cells, t)
            at = slice(t * LANES, t * LANES + keep)
            value = tile(t)
            before = tile(t - 1) if t > 0 else value
            after = tile(t + 1) if t < tiles - 1 else value
            west = jnp.where(lane == 0, turn(before, 1), turn(value, 1))
            east = jnp.where(lane == LANES - 1, turn(after, -1), turn(value, -1))
            south = jnp.where(lane < width, turn(before, width), turn(value, width))
            north = jnp.where(lane < wrap, turn(value, -width), turn(after, -width))
            for b, place, is_west, is_east in seams(width, t):
                rim = turn(jnp.where(lane < b, east_rim, west_rim), place - b)
                if is_west:
                    west = jnp.where(lane == place % LANES, rim, west)
                if is_east:
                    east = jnp.where(lane == (place - 1) % LANES, rim, east)
            if t * LANES < width:
                south = jnp.where(lane < width, south_rim, south)
            if (t + 1) * LANES > start:
                north = jnp.where(lane >= start - t * LANES, north_rim, north)
            flat = west + east + south + north - 4.0 * value
            above = jnp.concatenate([value[1:], value[levels - 1 :]], axis=0)
            below = jnp.concatenate([value[:1], value[: levels - 1]], axis=0)
            column = above + below - 2.0 * value
            updated = value + spread * flat + mixing * column
            out_ref[0, f, :, at] = wet_ref[0, :, at].astype(F32) * updated[:, :keep]
        return carry

    lax.fori_loop(0, fields, one_field, 0)


def cost(flops, moved):
    return pl.CostEstimate(flops=flops, bytes_accessed=moved, transcendentals=0)


def exchange(pack, groups, strips):
    def along(value, axis, size, step):
        return lax.ppermute(value, axis, [(i, (i + step) % size) for i in range(size)])

    beside = along(pack, "strip", strips, -1)
    if strips > 2:
        beside = jnp.concatenate([beside, along(pack, "strip", strips, 1)], axis=0)
    stack = jnp.concatenate([pack, beside], axis=0)
    return along(stack, "tiles", groups, 1), along(stack, "tiles", groups, -1), beside


def on_device(groups, strips, fields, wet_land, links, surface_diagonal, spread, mixing, thickness):
    field = fields[0, 0]
    slots, kinds, levels, cells = field.shape
    width = math.isqrt(cells)
    wet = wet_land.reshape(slots, 1, cells)
    diag = surface_diagonal.reshape(slots, 1, cells)
    seam = links[0, 0]
    depth = -(-(kinds * levels + 6) // SUBLANES) * SUBLANES
    bulk = 4 * field.size
    sides = 4 * slots

    def shape(*dims):
        return jax.ShapeDtypeStruct(dims, F32)

    def per_slot(count):
        return pl.BlockSpec((1, count, levels, cells), lambda s: (s, 0, 0, 0))

    line = pl.BlockSpec((1, 1, cells), lambda s: (s, 0, 0))
    rows = shape(width, SUBLANES, LANES)
    whole_rows = pl.BlockSpec((width, SUBLANES, LANES), lambda s: (0, 0, 0))
    params = pltpu.CompilerParams(vmem_limit_bytes=8 * 1024 * 1024)
    hbm = pl.BlockSpec(memory_space=pltpu.HBM)

    pack = pl.pallas_call(
        functools.partial(pack_kernel, width),
        in_specs=[SMEM, hbm, hbm, hbm],
        out_specs=VMEM,
        out_shape=pltpu.VMEM((sides, depth, LANES), F32),
        scratch_shapes=[pltpu.VMEM(field.shape, F32), pltpu.VMEM(wet.shape, jnp.int32), pltpu.VMEM(wet.shape, F32),
                        pltpu.VMEM((slots, depth, LANES), F32), pltpu.SemaphoreType.DMA((slots + 2,))],
        cost_estimate=cost(bulk, bulk),
        compiler_params=pltpu.CompilerParams(vmem_limit_bytes=58 * 1024 * 1024),
        name="pack_rims",
    )(thickness, field, wet, diag)
    up, down, beside = exchange(pack, groups, strips)

    u, v, wet_rows, diag_rows = pl.pallas_call(
        functools.partial(prepare_kernel, width),
        grid=(slots,),
        in_specs=[SMEM, per_slot(2), line, line],
        out_specs=[whole_rows] * 4,
        out_shape=[rows] * 4,
        scratch_shapes=[pltpu.VMEM((4, SUBLANES, tile_count(cells) * LANES), F32)],
        cost_estimate=cost(64 * bulk, bulk),
        compiler_params=params,
        name="prepare_rows",
    )(thickness, field, wet, diag)

    def local(kernel, outs, operands, name, scalars=0, scratch=()):
        return pl.pallas_call(
            kernel,
            in_specs=[SMEM] * scalars + [VMEM] * (len(operands) - scalars),
            out_specs=[VMEM] * len(outs),
            out_shape=outs,
            scratch_shapes=list(scratch),
            cost_estimate=cost(bulk, bulk),
            compiler_params=params,
            name=name,
        )(*operands)

    rims, kept, links_row = local(
        functools.partial(lines_kernel, width, strips),
        [shape(sides, kinds, levels, LANES), shape(4, 4 * SUBLANES, LANES), jax.ShapeDtypeStruct((1, LANES), jnp.int32)],
        [seam, thickness, up, down, beside, pack],
        "seam_lines",
        2,
        [pltpu.VMEM((12, 4 * SUBLANES, LANES), F32), pltpu.VMEM((3, 4 * SUBLANES, LANES), F32)],
    )
    (r,) = local(functools.partial(source_kernel, width), [rows], [kept, u, v, wet_rows], "source_rows")
    (q,) = local(functools.partial(operator_kernel, width, 1), [rows], [r, kept, diag_rows, wet_rows], "operator_rows")
    (w,) = local(functools.partial(operator_kernel, width, 2), [rows], [q, kept, diag_rows, wet_rows], "operator_rows")
    devices = groups * strips
    table, near = local(
        functools.partial(totals_kernel, width, slots),
        [shape(devices, 2, LANES), shape(1, LANES)],
        [kept, links_row, r, q, w, wet_rows, diag_rows],
        "partial_sums",
    )
    tables = lax.all_to_all(table, ("tiles", "strip"), 0, 0)

    updated = pl.pallas_call(
        functools.partial(slab_kernel, width),
        grid=(slots,),
        in_specs=[SMEM, SMEM, per_slot(kinds), line,
                  pl.BlockSpec((4, 1, kinds, levels, LANES), lambda s: (0, s, 0, 0, 0))],
        out_specs=per_slot(kinds),
        out_shape=shape(slots, kinds, levels, cells),
        scratch_shapes=[pltpu.VMEM((levels, tile_count(cells) * LANES), F32)],
        cost_estimate=cost(64 * bulk, 2 * bulk),
        compiler_params=params,
        name="slab_step",
    )(spread, mixing, field, wet, rims.reshape(4, slots, kinds, levels, LANES))

    surface = shape(slots, 1, cells)
    x, res = pl.pallas_call(
        functools.partial(finish_kernel, width, groups, strips),
        in_specs=[VMEM] * 6,
        out_specs=[VMEM] * 2,
        out_shape=[surface, surface],
        scratch_shapes=[pltpu.VMEM((width, SUBLANES, LANES), F32)] * 2,
        cost_estimate=cost(bulk, bulk),
        compiler_params=pltpu.CompilerParams(vmem_limit_bytes=(8 + devices // 64) * 1024 * 1024),
        name="finish",
    )(tables.reshape(2 * devices, LANES), near, r, q, w, wet_rows)
    return updated[None, None], x.reshape(1, 1, slots, cells), res.reshape(1, 1, slots, cells)


def solution(mesh):
    wide = P("tiles", "strip", None, None, None, None)
    flat = P("tiles", "strip", None, None)
    return jax.shard_map(
        functools.partial(on_device, mesh.shape["tiles"], mesh.shape["strip"]),
        mesh=mesh,
        in_specs=(wide, flat, P("tiles", "strip", None, None, None), flat, P(), P(), P()),
        out_specs=(wide, flat, flat),
        check_vma=False,
    )
```

```python
import functools
import math

import jax
import jax.numpy as jnp
from jax import lax
from jax.experimental import pallas as pl
from jax.experimental.pallas import tpu as pltpu
from jax.sharding import PartitionSpec as P

LANES = 128
SUBLANES = 8
ENDS = 8
F32 = jnp.float32
VMEM = pl.BlockSpec(memory_space=pltpu.VMEM)
SMEM = pl.BlockSpec(memory_space=pltpu.SMEM)


def lanes_of(rows):
    return lax.broadcasted_iota(jnp.int32, (rows, LANES), 1)


def rows_of(rows):
    return lax.broadcasted_iota(jnp.int32, (rows, LANES), 0)


def turn(value, shift):
    shift %= LANES
    return value if shift == 0 else pltpu.roll(value, shift, 1)


def take_lanes(value, index):
    return jnp.take_along_axis(value, index, axis=1, mode="promise_in_bounds")


def tile_count(cells):
    return -(-cells // LANES)


def tile_lanes(cells, tile):
    return min(LANES, cells - tile * LANES)


def seams(width, tile):
    found = []
    for b in range(width + 1):
        place = b * width
        west = b < width and place // LANES == tile
        east = b > 0 and (place - 1) // LANES == tile
        if west or east:
            found.append((b, place, west, east))
    return found


def side_lines(tile_of, rows, width, depth):
    cells = width * width
    lane = lanes_of(rows)
    zero = jnp.zeros((rows, LANES), F32)
    classes = 2 * depth
    kept = [zero] * classes
    for t in range(tile_count(cells)):
        for b in range(width + 1):
            place = b * width
            near = [
                o
                for o in range(-depth if b > 0 else 0, depth if b < width else 0)
                if (place + o) // LANES == t
            ]
            if near:
                inside = ((lane - (b + near[0])) & (LANES - 1)) < len(near)
                kept[b % classes] = jnp.where(inside, turn(tile_of(t), b - place), kept[b % classes])

    def straight(start):
        t, skip = divmod(start, LANES)
        value = turn(tile_of(t), -skip)
        if skip + width > LANES:
            value = jnp.where(lane < LANES - skip, value, turn(tile_of(t + 1), -skip))
        return jnp.where(lane < width, value, 0.0)

    west, east = [], []
    for d in range(depth):
        w, e = zero, zero
        for c in range(classes):
            w = jnp.where(lane % classes == c, turn(kept[c], -d), w)
            e = jnp.where((lane + 1) % classes == c, turn(kept[c], d), e)
        west.append(jnp.where(lane < width, w, 0.0))
        east.append(jnp.where(lane < width, e, 0.0))
    south = [straight(d * width) for d in range(depth)]
    north = [straight(cells - (d + 1) * width) for d in range(depth)]
    return west, east, south, north


def slope(value):
    return turn(value, -1) - turn(value, 1)


def place_of(side):
    return (0, 3, 1, 2)[side]


def pack_kernel(width, thick_ref, field_hbm, wet_hbm, diag_hbm, pack_ref, field_ref, wet_ref, diag_ref, tail_ref, flat_ref, lines_ref, sems):
    slots, fields, levels, cells = field_hbm.shape
    pair = 2 * levels
    copies = [pltpu.make_async_copy(wet_hbm, wet_ref, sems.at[0]), pltpu.make_async_copy(diag_hbm, diag_ref, sems.at[1])]
    copies += [pltpu.make_async_copy(field_hbm.at[k], field_ref.at[k], sems.at[2 + k]) for k in range(slots)]
    for copy in copies:
        copy.start()
    copies[0].wait()
    copies[1].wait()
    tiles = tile_count(cells)
    last = tiles - 1
    keep = tile_lanes(cells, last)
    base = fields * levels
    rows = rows_of(pair)
    weights = []
    for start in (0, levels):
        weight = jnp.zeros((pair, LANES), F32)
        for l in range(levels):
            weight = jnp.where(rows == start + l, 0.5 * thick_ref[l], weight)
        weights.append(weight)
    flat_ref[:, last * LANES :] = jnp.zeros((2 * SUBLANES, LANES), F32)
    for t in range(tiles):
        at = slice(t * LANES, t * LANES + tile_lanes(cells, t))
        for k in range(slots):
            flat_ref[k : k + 1, at] = wet_ref[k, :, at].astype(F32)
            flat_ref[SUBLANES + k : SUBLANES + k + 1, at] = diag_ref[k, :, at]
    wet = side_lines(lambda t: flat_ref[:SUBLANES, t * LANES : (t + 1) * LANES], SUBLANES, width, 3)
    diag = side_lines(lambda t: flat_ref[SUBLANES:, t * LANES : (t + 1) * LANES], SUBLANES, width, 1)
    tail_ref[...] = jnp.zeros_like(tail_ref)
    lines_ref[...] = jnp.zeros_like(lines_ref)

    def piece(k, f, t):
        if t < last:
            return field_ref[k, f, :, t * LANES : (t + 1) * LANES]
        return tail_ref[k, f]

    def joined(first, second):
        made = {}

        def tile_of(t):
            if t not in made:
                made.clear()
                made[t] = jnp.concatenate([piece(*first, t), piece(*second, t)], axis=0)
            return made[t]

        return tile_of

    for k in range(slots):
        copies[2 + k].wait()
        for f in range(fields):
            tail_ref[k, f, :, :keep] = field_ref[k, f, :, last * LANES : cells]
        both = side_lines(joined((k, 0), (k, 1)), pair, width, 3)
        for e in range(4):
            at = place_of(e) * slots + k
            mask = [wet[e][d][k : k + 1] for d in range(3)]
            pack_ref[at, :pair, :] = both[e][0] * mask[0]
            normal, along = weights if e < 2 else weights[::-1]
            line = slice(e * SUBLANES + k, e * SUBLANES + k + 1)
            for n, (weight, d) in enumerate(((normal, 0), (normal, 1), (normal, 2), (along, 0), (along, 1))):
                lines_ref[n, line, :] = jnp.sum(both[e][d] * weight, axis=0, keepdims=True) * mask[d]
            lines_ref[5, line, :] = mask[0]
            lines_ref[6, line, :] = mask[1]
    normal1, normal2, normal3, along1, along2, wet1, wet2 = (lines_ref[n] for n in range(7))
    inward = jnp.where((rows_of(4 * SUBLANES) // SUBLANES) % 2 == 0, 1.0, -1.0)
    first = wet1 * (inward * normal2 + slope(along1))
    second = wet2 * (inward * (normal3 - normal1) + slope(along2))
    for e in range(4):
        for k in range(slots):
            at = place_of(e) * slots + k
            line = slice(e * SUBLANES + k, e * SUBLANES + k + 1)
            extra = (wet1[line], diag[e][0][k : k + 1], first[line], second[line])
            for n, value in enumerate(extra):
                pack_ref[at, base + n : base + n + 1, :] = value
    scalars = [(k, f) for k in range(slots) for f in range(2, fields)]
    for n in range(0, len(scalars), 2):
        two = scalars[n : n + 2]
        lines = side_lines(joined(two[0], two[-1]), pair, width, 1)
        for m, (k, f) in enumerate(two):
            for e in range(4):
                value = lines[e][0][m * levels : (m + 1) * levels] * wet[e][0][k : k + 1]
                pack_ref[place_of(e) * slots + k, f * levels : (f + 1) * levels, :] = value


def to_rows(flat_ref, out_ref, width, masked):
    lane = lanes_of(SUBLANES)
    for i in range(width):
        t, skip = divmod(i * width, LANES)
        row = turn(flat_ref[:, t * LANES : (t + 1) * LANES], -skip)
        if skip + width > LANES:
            rest = turn(flat_ref[:, (t + 1) * LANES : (t + 2) * LANES], -skip)
            row = jnp.where(lane < LANES - skip, row, rest)
        if masked:
            row = jnp.where(lane < width, row, 0.0)
        out_ref[i] = row


def prepare_kernel(width, thick_ref, field_ref, wet_ref, diag_ref, u_ref, v_ref, wet_rows_ref, diag_rows_ref, flat_ref):
    _, _, levels, cells = field_ref.shape
    slot = pl.program_id(0)
    rows = rows_of(levels)
    weight = jnp.zeros((levels, LANES), F32)
    for l in range(levels):
        weight = jnp.where(rows == l, 0.5 * thick_ref[l], weight)

    @pl.when(slot == 0)
    def _():
        flat_ref[...] = jnp.zeros_like(flat_ref)

    for t in range(tile_count(cells)):
        keep = tile_lanes(cells, t)
        at = slice(t * LANES, t * LANES + keep)
        wet = wet_ref[0, :, at].astype(F32)
        factor = weight[:, :keep] * wet
        terms = (
            jnp.sum(field_ref[0, 0, :, at] * factor, axis=0, keepdims=True),
            jnp.sum(field_ref[0, 1, :, at] * factor, axis=0, keepdims=True),
            wet,
            diag_ref[0, :, at],
        )
        mine = rows_of(SUBLANES)[:, :keep] == slot
        for n, term in enumerate(terms):
            flat_ref[n, :, at] = jnp.where(mine, term, flat_ref[n, :, at])

    @pl.when(slot == pl.num_programs(0) - 1)
    def _():
        to_rows(flat_ref.at[0], u_ref, width, False)
        to_rows(flat_ref.at[1], v_ref, width, False)
        to_rows(flat_ref.at[2], wet_rows_ref, width, True)
        to_rows(flat_ref.at[3], diag_rows_ref, width, False)


def strip_place(shift, strips):
    return jnp.bitwise_and(shift, 1) if strips == 2 else jnp.where(shift < 0, 2, shift)


def partner_block(links_ref, k, e, strips, slots, up_ref, down_ref, beside_ref):
    group_shift = links_ref[k, e, 0]
    place = strip_place(links_ref[k, e, 1], strips)
    partner = jnp.maximum(links_ref[k, e, 2], 0)
    strip = jnp.maximum(place - 1, 0)
    whole = 4 * slots
    most = whole - slots
    entry = place_of(e ^ 1) * slots + partner
    from_up = slots + strip * most + entry - slots
    from_down = slots + strip * most + entry
    if e == 0:
        return up_ref[jnp.where(place == 0, partner, from_up)]
    if e == 1:
        return down_ref[jnp.where(place == 0, partner, from_down)]
    upper = (group_shift < 0).astype(F32)
    lower = (group_shift > 0).astype(F32)
    middle = 1.0 - upper - lower
    return upper * up_ref[from_up] + lower * down_ref[from_down] + middle * beside_ref[strip * whole + entry]


def seam_numbers(links_ref, k, e):
    code = links_ref[k, e, 3]
    live = (links_ref[k, e, 2] >= 0).astype(F32)
    cosine = (code == 0).astype(F32) - (code == 2).astype(F32)
    sine = (code == 1).astype(F32) - (code == 3).astype(F32)
    return (code != 0).astype(jnp.int32), live, cosine, sine


def backward_step(lane, width):
    return jnp.where(lane < width, width - 1 - 2 * lane, 0)


def side_columns(lines_ref, width):
    lane = lanes_of(SUBLANES)
    west = lines_ref[0:SUBLANES, :]
    east = turn(lines_ref[SUBLANES : 2 * SUBLANES, :], width - 1)

    def column(i):
        return turn(jnp.where(lane == i, west, east), -i)

    return column


def operator_rows(x_ref, lines_ref, diag_ref, wet_ref, out_ref, width):
    lane = lanes_of(SUBLANES)
    column = side_columns(lines_ref, width)
    for i in range(width):
        x = x_ref[i]
        ends = column(i)
        west = jnp.where(lane == 0, ends, turn(x, 1))
        east = jnp.where(lane == width - 1, ends, turn(x, -1))
        south = x_ref[i - 1] if i > 0 else lines_ref[2 * SUBLANES : 3 * SUBLANES, :]
        north = x_ref[i + 1] if i < width - 1 else lines_ref[3 * SUBLANES : 4 * SUBLANES, :]
        out_ref[i] = wet_ref[i] * ((4.0 + diag_ref[i]) * x - (west + east + south + north))


def dotted(a_ref, b_ref, width, chunk=10):
    total = None
    for start in range(0, width, chunk):
        part = None
        for i in range(start, min(start + chunk, width)):
            term = a_ref[i] * b_ref[i]
            part = term if part is None else part + term
        total = part if total is None else total + part
    return jnp.sum(total, axis=(0, 1), keepdims=True)


def lines_kernel(width, strips, links_ref, thick_ref, spread_ref, up_ref, down_ref, beside_ref, own_ref,
                 rims_ref, kept_ref, table_ref, lines_ref, numbers_ref):
    slots = links_ref.shape[0]
    fields, levels = spread_ref.shape
    depth = up_ref.shape[1]
    pair = 2 * levels
    base = fields * levels
    stride = slots * ENDS
    lane_all = lanes_of(depth)
    mirror = backward_step(lane_all, width)
    rows = rows_of(pair)
    sign = jnp.where(rows < levels, 1.0, -1.0)
    weights = []
    for start in (0, levels):
        weight = jnp.zeros((pair, LANES), F32)
        for l in range(levels):
            weight = jnp.where(rows == start + l, 0.5 * thick_ref[l], weight)
        weights.append(weight)
    places = 2 if strips == 2 else 3
    lane1 = lanes_of(1)
    lines_ref[...] = jnp.zeros_like(lines_ref)
    numbers_ref[...] = jnp.zeros_like(numbers_ref)
    code_ref = table_ref
    spreads = field_levels(spread_ref, rims_ref.shape[1])
    table = jnp.full((1, LANES), -1, jnp.int32)
    ends = [(e, k) for e in range(4) for k in range(slots)]
    numbers = {at: seam_numbers(links_ref, at[1], at[0]) for at in ends}
    blocks = {at: partner_block(links_ref, at[1], at[0], strips, slots, up_ref, down_ref, beside_ref) for at in ends}
    for at in ends:
        flip, live, _, _ = numbers[at]
        blocks[at] = take_lanes(blocks[at], lane_all + flip * mirror) * live

    def summed(value, weight):
        return jnp.sum(value * weight, axis=0, keepdims=True)

    for at in ends:
        e, k = at
        flip, live, cosine, sine = numbers[at]
        block = blocks[at]
        both = block[:pair]
        turned = cosine * both + (sine * sign) * pltpu.roll(both, levels, 0)
        side = e * slots + k
        mine = place_of(e) * slots + k
        here = own_ref[mine, base : base + 1, :]
        rims_ref[side, :pair] = turned * spreads[:pair] * here
        rims_ref[side, pair:base] = block[pair:base] * spreads[pair:base] * here
        rims_ref[side, base:] = jnp.zeros((rims_ref.shape[1] - base, LANES), F32)
        line = slice(e * SUBLANES + k, e * SUBLANES + k + 1)
        for n in range(4):
            lines_ref[n, line, :] = block[base + n : base + n + 1]
        normal, along = weights if e < 2 else weights[::-1]
        inner = own_ref[mine, :pair, :]
        lines_ref[4, line, :] = summed(both, normal)
        lines_ref[5, line, :] = summed(both, along)
        lines_ref[6, line, :] = summed(inner, normal)
        lines_ref[7, line, :] = summed(inner, along)
        lines_ref[8, line, :] = here
        lines_ref[9, line, :] = own_ref[mine, base + 2 : base + 3, :]
        numbers_ref[0, line, :] = jnp.full((1, LANES), cosine, F32)
        numbers_ref[1, line, :] = jnp.full((1, LANES), sine if e < 2 else -sine, F32)
        partner = links_ref[k, e, 2]
        near = (links_ref[k, e, 0] + 1) * places + strip_place(links_ref[k, e, 1], strips)
        for end in range(2):
            from_lane = partner * ENDS + (e ^ 1) * 2 + (end + flip - 2 * end * flip)
            entry = jnp.where(partner >= 0, near * 32 + from_lane, -1)
            table = jnp.where(lane1 == k * ENDS + e * 2 + end, entry, table)

    wet1, diag1, first, second, normal1, along1, normal0, along0, wet0, own = (lines_ref[n] for n in range(10))
    cosine, sine = numbers_ref[0], numbers_ref[1]
    received = cosine * normal1 + sine * along1
    given = cosine * normal0 - sine * along0
    outward = jnp.where((rows_of(4 * SUBLANES) // SUBLANES) % 2 == 0, 1.0, -1.0)
    first = first + wet1 * (outward * given)
    lane8 = lanes_of(SUBLANES)

    def at_ends(e):
        low, high = (2, 3) if e < 2 else (0, 1)
        place = jnp.full((SUBLANES, LANES), (e % 2) * (width - 1), jnp.int32)
        before = take_lanes(received[low * SUBLANES : (low + 1) * SUBLANES], place)
        after = take_lanes(received[high * SUBLANES : (high + 1) * SUBLANES], place)
        return jnp.where(lane8 == 0, -before, jnp.where(lane8 == width - 1, after, 0.0))

    lateral = jnp.concatenate([at_ends(e) for e in range(4)], axis=0)
    own = own + wet0 * (lateral - outward * received)
    beside = second + own + turn(first, 1) + turn(first, -1)
    far = wet1 * ((4.0 + diag1) * first - beside)
    for n, value in enumerate((received, first, far, wet1)):
        kept_ref[n] = value
    code_ref[...] = table


def source_kernel(width, kept_ref, u_ref, v_ref, wet_ref, r_ref):
    lane = lanes_of(SUBLANES)
    column = side_columns(kept_ref.at[0], width)
    for i in range(width):
        across = u_ref[i]
        cells = column(i)
        west = jnp.where(lane == 0, cells, turn(across, 1))
        east = jnp.where(lane == width - 1, cells, turn(across, -1))
        south = v_ref[i - 1] if i > 0 else kept_ref[0, 2 * SUBLANES : 3 * SUBLANES, :]
        north = v_ref[i + 1] if i < width - 1 else kept_ref[0, 3 * SUBLANES : 4 * SUBLANES, :]
        r_ref[i] = wet_ref[i] * (east - west + north - south)


def operator_kernel(width, line, x_ref, kept_ref, diag_ref, wet_ref, out_ref):
    operator_rows(x_ref, kept_ref.at[line], diag_ref, wet_ref, out_ref, width)


def totals_kernel(width, slots, kept_ref, table_ref, r_ref, q_ref, w_ref, wet_ref, diag_ref, rows_ref, near_ref):
    stride = slots * ENDS
    lane1 = lanes_of(1)
    lane = lanes_of(SUBLANES)
    first, far, wet1 = kept_ref[1], kept_ref[2], kept_ref[3]
    table = table_ref[...]
    block_of = rows_of(SUBLANES) == lane // ENDS
    which = lane % ENDS
    side = which // 2
    end = which % 2
    upright = side < 2
    column = jnp.where(upright, side, end) * (width - 1)
    upper = jnp.where(upright, end, side - 2) == 1
    step = 1 + end * (width - 3)
    beside_column = jnp.where(upright, column, step)

    def in_row(value):
        value = jnp.sum(jnp.where(block_of, value, 0.0), axis=0, keepdims=True)
        return jnp.where(lane1 < stride, value, 0.0)

    def corners(ref):
        return in_row(jnp.where(upper, take_lanes(ref[width - 1], column), take_lanes(ref[0], column)))

    def of_lines(value, index):
        total = jnp.zeros((SUBLANES, LANES), F32)
        for e in range(4):
            total = jnp.where(side == e, take_lanes(value[e * SUBLANES : (e + 1) * SUBLANES], index), total)
        return in_row(total)

    lower_row = jnp.where(upright, take_lanes(q_ref[1], beside_column), take_lanes(q_ref[0], beside_column))
    upper_row = jnp.where(upright, take_lanes(q_ref[width - 2], beside_column), take_lanes(q_ref[width - 1], beside_column))
    q_next = in_row(jnp.where(upper, upper_row, lower_row))
    q_corner = corners(q_ref)
    near = of_lines(wet1, step)
    near_ref[...] = near
    sums = (dotted(r_ref, r_ref, width), dotted(r_ref, q_ref, width), dotted(q_ref, q_ref, width), dotted(q_ref, w_ref, width))
    total = jnp.zeros((1, LANES), F32)
    for n, value in enumerate(sums):
        total = jnp.where(lane1 == n, value, total)
    last = end * (width - 1)
    code = jnp.where(lane1 < stride, table, 0).astype(F32)
    diag_corner = corners(diag_ref)
    made = []
    for values in (
        (corners(r_ref), of_lines(first, last), q_corner, of_lines(far, last), code),
        (corners(wet_ref), q_next * near - corners(w_ref), q_next, 4.0 + diag_corner, total),
    ):
        row = jnp.zeros((1, LANES), F32)
        for m, value in enumerate(values):
            row = jnp.where((lane1 >= m * stride) & (lane1 < (m + 1) * stride), turn(value, m * stride), row)
        made.append(row)
    both = jnp.where(rows_of(SUBLANES) % 2 == 0, made[0], made[1])
    for start in range(0, rows_ref.shape[0], SUBLANES):
        rows_ref[start : start + SUBLANES, :] = both


def finish_kernel(width, groups, strips, tables_ref, near_ref, r_ref, q_ref, w_ref, wet_ref, x_ref, res_ref, sol_rows, res_rows):
    devices = groups * strips
    slots, _, cells = x_ref.shape
    stride = slots * ENDS
    lane = lanes_of(devices)
    row = rows_of(devices)
    me = lax.axis_index("tiles") * strips + lax.axis_index("strip")
    strip = row % strips
    tables = [tables_ref[pl.ds(n, devices, stride=2), :] for n in range(2)]
    listed = lane < stride

    def part(n, m):
        return jnp.where(listed, turn(tables[n], -m * stride), 0.0)

    r_corner, first_seen, q_seen, far_seen, code = (part(0, m) for m in range(5))
    wet_corner, mixed, q_next, diag_corner, totals = (part(1, m) for m in range(5))
    link = jnp.where(listed, code, -1.0).astype(jnp.int32)
    near = jnp.where(link < 0, -1, link // 32)
    from_lane = jnp.where(link < 0, 0, link % 32)

    def by_rows(value, shift):
        shift %= devices
        return value if shift == 0 else pltpu.roll(value, shift, 0)

    shifts = (0, 1) if strips == 2 else (0, 1, -1)

    def from_partner(value):
        found = jnp.zeros_like(value)
        for group_shift in (-1, 0, 1):
            shifted = by_rows(value, -group_shift * strips)
            for place, strip_shift in enumerate(shifts):
                if group_shift == 0 and strip_shift == 0:
                    continue
                if strip_shift == 0:
                    there = shifted
                elif strip_shift == 1:
                    there = jnp.where(strip < strips - 1, by_rows(shifted, -1), by_rows(shifted, strips - 1))
                else:
                    there = jnp.where(strip > 0, by_rows(shifted, 1), by_rows(shifted, 1 - strips))
                taken = take_lanes(there, from_lane)
                found = jnp.where(near == (group_shift + 1) * len(shifts) + place, taken, found)
        return found

    rise = jnp.where(near >= 0, from_partner(r_corner) - first_seen, 0.0)
    which = lane % ENDS
    other = lane - which + (1 - which // 4) * 4 + (which % 2) * 2 + (which // 2) % 2
    at_corner = rise + take_lanes(rise, other)
    change = -wet_corner * at_corner
    q_corner = q_seen + change
    excess = jnp.where(near >= 0, from_partner(q_corner) - far_seen, 0.0)

    def overall(value):
        return jnp.sum(value, axis=(0, 1), keepdims=True)

    sums = jnp.sum(totals, axis=0, keepdims=True)
    lane1 = lanes_of(1)
    rr, rq, qq, qw = (jnp.sum(jnp.where(lane1 == n, sums, 0.0), axis=1, keepdims=True) for n in range(4))
    rq = rq - overall(r_corner * rise)
    qq = qq + overall(0.5 * wet_corner * at_corner * at_corner - 2.0 * q_seen * rise)
    qw = qw + overall(rise * mixed + q_corner * (0.5 * diag_corner * change - excess) - q_next * change)
    alpha = rr / rq
    next_rr = rr - 2.0 * alpha * rq + alpha * alpha * qq
    image = rq - 2.0 * alpha * qq + alpha * alpha * qw
    ratio = next_rr / rr
    second = next_rr / (image - ratio * next_rr / alpha)

    lane8 = lanes_of(SUBLANES)
    slot8 = rows_of(SUBLANES) * ENDS

    def own(value):
        value = jnp.sum(jnp.where(row == me, value, 0.0), axis=0, keepdims=True)
        return jnp.broadcast_to(value, (SUBLANES, LANES))

    own_change = own(change)
    at_corners = own(0.5 * diag_corner * change - excess)
    at_next = jnp.broadcast_to(near_ref[...], (SUBLANES, LANES)) * own(rise) - own_change

    def entry(value, n):
        return take_lanes(value, slot8 + n)

    def placed(values):
        total = jnp.zeros((SUBLANES, LANES), F32)
        for at, value in values:
            total = jnp.where(lane8 == at, value, total)
        return total

    w_change = {
        0: ((0, entry(at_corners, 0) + entry(at_corners, 4)), (width - 1, entry(at_corners, 2) + entry(at_corners, 5)),
            (1, entry(at_next, 4)), (width - 2, entry(at_next, 5))),
        1: ((0, entry(at_next, 0)), (width - 1, entry(at_next, 2))),
        width - 2: ((0, entry(at_next, 1)), (width - 1, entry(at_next, 3))),
        width - 1: ((0, entry(at_corners, 1) + entry(at_corners, 6)), (width - 1, entry(at_corners, 3) + entry(at_corners, 7)),
                    (1, entry(at_next, 6)), (width - 2, entry(at_next, 7))),
    }
    q_change = {
        0: ((0, entry(own_change, 0)), (width - 1, entry(own_change, 2))),
        width - 1: ((0, entry(own_change, 1)), (width - 1, entry(own_change, 3))),
    }
    for i in range(width):
        r = r_ref[i]
        q = q_ref[i]
        w = w_ref[i]
        if i in q_change:
            q = q + placed(q_change[i])
        if i in w_change:
            w = w + wet_ref[i] * placed(w_change[i])
        residual = r - alpha * q
        direction = residual + ratio * r
        sol_rows[i] = alpha * r + second * direction
        res_rows[i] = residual - second * (q - alpha * w + ratio * q)
    for rows_from, out_ref in ((sol_rows, x_ref), (res_rows, res_ref)):
        for t in range(tile_count(cells)):
            keep = tile_lanes(cells, t)
            value = None
            for i in range(t * LANES // width, (t * LANES + keep - 1) // width + 1):
                start = i * width - t * LANES
                piece = turn(rows_from[i], start)
                value = piece if value is None else jnp.where(lane8 >= start, piece, value)
            for k in range(slots):
                out_ref[k, :, t * LANES : t * LANES + keep] = value[k : k + 1, :keep]


def field_levels(spread_ref, count):
    fields, levels = spread_ref.shape
    rows = rows_of(count)
    value = jnp.zeros((count, LANES), F32)
    for f in range(fields):
        for l in range(levels):
            value = jnp.where(rows == f * levels + l, spread_ref[f, l], value)
    return value


def slab_kernel(width, spread_ref, mixing_ref, field_ref, wet_ref, rims_ref, out_ref, masked_ref, wet_row_ref):
    _, fields, levels, cells = field_ref.shape
    count = masked_ref.shape[0]
    tiles = tile_count(cells)
    lane = lanes_of(SUBLANES)
    level = rows_of(SUBLANES) % levels
    tail = tiles - 1
    masked_ref[:, tail * LANES :] = jnp.zeros((count, LANES), F32)
    if count > fields * levels:
        masked_ref[fields * levels :, :] = jnp.zeros((count - fields * levels, tiles * LANES), F32)
    wet_row_ref[:, tail * LANES :] = jnp.zeros((1, LANES), F32)
    for t in range(tiles):
        at = slice(t * LANES, t * LANES + tile_lanes(cells, t))
        wet = wet_ref[0, :, at].astype(F32)
        wet_row_ref[:, at] = wet
        for f in range(fields):
            masked_ref[f * levels : (f + 1) * levels, at] = field_ref[0, f, :, at] * wet
    spreads = field_levels(spread_ref, count)
    mixing = jnp.zeros((SUBLANES, LANES), F32)
    for l in range(levels):
        mixing = jnp.where(level == l, mixing_ref[l], mixing)
    per = SUBLANES // levels
    first = cells - width
    corner, skip = divmod(first, LANES)
    zero = jnp.zeros((SUBLANES, LANES), F32)
    for start in range(0, count, SUBLANES):
        spread = spreads[start : start + SUBLANES]
        west_rim, east_rim, south_rim, north_rim = (rims_ref[e, 0, start : start + SUBLANES, :] for e in range(4))
        north_rim = turn(north_rim, first)

        def tile(t):
            if t < 0 or t >= tiles:
                return zero
            return masked_ref[start : start + SUBLANES, t * LANES : (t + 1) * LANES]

        for t in range(tiles):
            keep = tile_lanes(cells, t)
            value = tile(t)
            west = jnp.where(lane == 0, turn(tile(t - 1), 1), turn(value, 1))
            east = jnp.where(lane == LANES - 1, turn(tile(t + 1), -1), turn(value, -1))
            south = jnp.where(lane < width, turn(tile(t - 1), width), turn(value, width))
            north = jnp.where(lane < LANES - width, turn(value, -width), turn(tile(t + 1), -width))
            added = zero
            for b, at, is_west, is_east in seams(width, t):
                line = zero
                if is_west:
                    west = jnp.where(lane == at % LANES, 0.0, west)
                    line = jnp.where(lane == b, west_rim, line)
                if is_east:
                    east = jnp.where(lane == (at - 1) % LANES, 0.0, east)
                    line = jnp.where(lane == b - 1, east_rim, line)
                added = added + turn(line, at - b)
            if t == 0:
                added = added + south_rim
            if t == corner:
                added = added + jnp.where(lane >= skip, north_rim, 0.0)
            if t == corner + 1:
                added = added + jnp.where(lane < skip, north_rim, 0.0)
            flat = west + east + south + north - 4.0 * value
            above = jnp.where(level == levels - 1, value, pltpu.roll(value, SUBLANES - 1, 0))
            below = jnp.where(level == 0, value, pltpu.roll(value, 1, 0))
            updated = value + spread * flat + mixing * (above + below - 2.0 * value)
            updated = wet_row_ref[:, t * LANES : (t + 1) * LANES] * updated + added
            for n in range(per):
                f = start // levels + n
                if f < fields:
                    out_ref[0, f, :, t * LANES : t * LANES + keep] = updated[n * levels : (n + 1) * levels, :keep]


def cost(flops, moved):
    return pl.CostEstimate(flops=flops, bytes_accessed=moved, transcendentals=0)


def exchange(pack, slots, groups, strips):
    def along(value, axis, size, step):
        return lax.ppermute(value, axis, [(i, (i + step) % size) for i in range(size)])

    beside = [along(pack, "strip", strips, -1)]
    if strips > 2:
        beside.append(along(pack, "strip", strips, 1))
    to_up = jnp.concatenate([pack[3 * slots :]] + [b[slots:] for b in beside], axis=0)
    to_down = jnp.concatenate([pack[:slots]] + [b[: 3 * slots] for b in beside], axis=0)
    beside = jnp.concatenate(beside, axis=0) if strips > 2 else beside[0]
    even = lax.axis_index("tiles") % 2 == 0
    near = lax.ppermute(jnp.where(even, to_up, to_down), "tiles", [(i, i ^ 1) for i in range(groups)])
    far = lax.ppermute(
        jnp.where(even, to_down, to_up), "tiles", [(i, (i + 1 if i % 2 else i - 1) % groups) for i in range(groups)]
    )
    return jnp.where(even, far, near), jnp.where(even, near, far), beside


def on_device(groups, strips, fields, wet_land, links, surface_diagonal, spread, mixing, thickness):
    field = fields[0, 0]
    slots, kinds, levels, cells = field.shape
    width = math.isqrt(cells)
    wet = wet_land.reshape(slots, 1, cells)
    diag = surface_diagonal.reshape(slots, 1, cells)
    seam = links[0, 0]
    depth = -(-(kinds * levels + 4) // SUBLANES) * SUBLANES
    bulk = 4 * field.size
    sides = 4 * slots

    def shape(*dims):
        return jax.ShapeDtypeStruct(dims, F32)

    def per_slot(count):
        return pl.BlockSpec((1, count, levels, cells), lambda s: (s, 0, 0, 0))

    line = pl.BlockSpec((1, 1, cells), lambda s: (s, 0, 0))
    rows = shape(width, SUBLANES, LANES)
    whole_rows = pl.BlockSpec((width, SUBLANES, LANES), lambda s: (0, 0, 0))
    params = pltpu.CompilerParams(vmem_limit_bytes=8 * 1024 * 1024)
    hbm = pl.BlockSpec(memory_space=pltpu.HBM)

    pack = pl.pallas_call(
        functools.partial(pack_kernel, width),
        in_specs=[SMEM, hbm, hbm, hbm],
        out_specs=VMEM,
        out_shape=pltpu.VMEM((sides, depth, LANES), F32),
        scratch_shapes=[pltpu.VMEM(field.shape, F32), pltpu.VMEM(wet.shape, jnp.int32), pltpu.VMEM(wet.shape, F32),
                        pltpu.VMEM((slots, kinds, levels, LANES), F32), pltpu.VMEM((2 * SUBLANES, tile_count(cells) * LANES), F32),
                        pltpu.VMEM((7, 4 * SUBLANES, LANES), F32), pltpu.SemaphoreType.DMA((slots + 2,))],
        cost_estimate=cost(bulk, bulk),
        compiler_params=pltpu.CompilerParams(vmem_limit_bytes=58 * 1024 * 1024),
        name="pack_rims",
    )(thickness, field, wet, diag)
    up, down, beside = exchange(pack, slots, groups, strips)

    slab_rows = -(-kinds * levels // SUBLANES) * SUBLANES
    flat_lanes = tile_count(cells) * LANES
    u, v, wet_rows, diag_rows = pl.pallas_call(
        functools.partial(prepare_kernel, width),
        grid=(slots,),
        in_specs=[SMEM, per_slot(2), line, line],
        out_specs=[whole_rows] * 4,
        out_shape=[rows] * 4,
        scratch_shapes=[pltpu.VMEM((4, SUBLANES, flat_lanes), F32)],
        cost_estimate=cost(64 * bulk, bulk),
        compiler_params=params,
        name="prepare_rows",
    )(thickness, field, wet, diag)

    def local(kernel, outs, operands, name, scalars=0, scratch=()):
        return pl.pallas_call(
            kernel,
            in_specs=[SMEM] * scalars + [VMEM] * (len(operands) - scalars),
            out_specs=[VMEM] * len(outs),
            out_shape=outs,
            scratch_shapes=list(scratch),
            cost_estimate=cost(bulk, bulk),
            compiler_params=params,
            name=name,
        )(*operands)

    rims, kept, links_row = local(
        functools.partial(lines_kernel, width, strips),
        [shape(sides, slab_rows, LANES), shape(4, 4 * SUBLANES, LANES), jax.ShapeDtypeStruct((1, LANES), jnp.int32)],
        [seam, thickness, spread, up, down, beside, pack],
        "seam_lines",
        3,
        [pltpu.VMEM((10, 4 * SUBLANES, LANES), F32), pltpu.VMEM((2, 4 * SUBLANES, LANES), F32)],
    )
    (r,) = local(functools.partial(source_kernel, width), [rows], [kept, u, v, wet_rows], "source_rows")
    (q,) = local(functools.partial(operator_kernel, width, 1), [rows], [r, kept, diag_rows, wet_rows], "operator_rows")
    (w,) = local(functools.partial(operator_kernel, width, 2), [rows], [q, kept, diag_rows, wet_rows], "operator_rows")
    devices = groups * strips
    table, near = local(
        functools.partial(totals_kernel, width, slots),
        [pltpu.VMEM((2 * devices, LANES), F32), shape(1, LANES)],
        [kept, links_row, r, q, w, wet_rows, diag_rows],
        "partial_sums",
    )
    tables = lax.all_to_all(table.reshape(devices, 2, LANES), ("tiles", "strip"), 0, 0)

    updated = pl.pallas_call(
        functools.partial(slab_kernel, width),
        grid=(slots,),
        in_specs=[SMEM, SMEM, per_slot(kinds), line, pl.BlockSpec((4, 1, slab_rows, LANES), lambda s: (0, s, 0, 0))],
        out_specs=per_slot(kinds),
        out_shape=shape(slots, kinds, levels, cells),
        scratch_shapes=[pltpu.VMEM((slab_rows, flat_lanes), F32), pltpu.VMEM((1, flat_lanes), F32)],
        cost_estimate=cost(64 * bulk, 2 * bulk),
        compiler_params=params,
        name="slab_step",
    )(spread, mixing, field, wet, rims.reshape(4, slots, slab_rows, LANES))

    surface = shape(slots, 1, cells)
    x, res = pl.pallas_call(
        functools.partial(finish_kernel, width, groups, strips),
        in_specs=[VMEM] * 6,
        out_specs=[VMEM] * 2,
        out_shape=[surface, surface],
        scratch_shapes=[pltpu.VMEM((width, SUBLANES, LANES), F32)] * 2,
        cost_estimate=cost(bulk, bulk),
        compiler_params=pltpu.CompilerParams(vmem_limit_bytes=(8 + devices // 64) * 1024 * 1024),
        name="finish",
    )(tables.reshape(2 * devices, LANES), near, r, q, w, wet_rows)
    return updated[None, None], x.reshape(1, 1, slots, cells), res.reshape(1, 1, slots, cells)


def solution(mesh):
    wide = P("tiles", "strip", None, None, None, None)
    flat = P("tiles", "strip", None, None)
    return jax.shard_map(
        functools.partial(on_device, mesh.shape["tiles"], mesh.shape["strip"]),
        mesh=mesh,
        in_specs=(wide, flat, P("tiles", "strip", None, None, None), flat, P(), P(), P()),
        out_specs=(wide, flat, flat),
        check_vma=False,
    )
```

```python
import functools
import math

import jax
import jax.numpy as jnp
from jax import lax
from jax.experimental import pallas as pl
from jax.experimental.pallas import tpu as pltpu
from jax.sharding import PartitionSpec as P


LANES = 128
SUBLANES = 8
ENDS = 8
F32 = jnp.float32
VMEM = pl.BlockSpec(memory_space=pltpu.VMEM)
SMEM = pl.BlockSpec(memory_space=pltpu.SMEM)


def lanes_of(rows):
    return lax.broadcasted_iota(jnp.int32, (rows, LANES), 1)


def rows_of(rows):
    return lax.broadcasted_iota(jnp.int32, (rows, LANES), 0)


def turn(value, shift):
    shift %= LANES
    return value if shift == 0 else pltpu.roll(value, shift, 1)


def take_lanes(value, index):
    return jnp.take_along_axis(value, index, axis=1, mode="promise_in_bounds")


def fold_of(width, slots):
    return 2 if width % 2 == 0 and 2 * slots <= SUBLANES else 1


def lifted(value, count):
    count %= SUBLANES
    return value if count == 0 else pltpu.roll(value, count, 0)


def row_at(ref, i, slots):
    count = ref.shape[0]
    return ref[i] if i < count else lifted(ref[i - count], -slots)


def row_south(ref, line, i, slots, fold):
    if i > 0:
        return ref[i - 1]
    if fold == 1:
        return line
    return jnp.where(rows_of(SUBLANES) < slots, line, lifted(ref[ref.shape[0] - 1], slots))


def row_north(ref, line, i, slots, fold):
    if i < ref.shape[0] - 1:
        return ref[i + 1]
    if fold == 1:
        return line
    return jnp.where(rows_of(SUBLANES) < slots, lifted(ref[0], -slots), lifted(line, slots))


def tile_count(cells):
    return -(-cells // LANES)


def tile_lanes(cells, tile):
    return min(LANES, cells - tile * LANES)


def seams(width, tile):
    found = []
    for b in range(width + 1):
        place = b * width
        west = b < width and place // LANES == tile
        east = b > 0 and (place - 1) // LANES == tile
        if west or east:
            found.append((b, place, west, east))
    return found


def side_lines(tile_of, rows, width, depth):
    cells = width * width
    lane = lanes_of(rows)
    zero = jnp.zeros((rows, LANES), F32)
    classes = 2 * depth
    kept = [zero] * classes
    for t in range(tile_count(cells)):
        for b in range(width + 1):
            place = b * width
            near = [
                o
                for o in range(-depth if b > 0 else 0, depth if b < width else 0)
                if (place + o) // LANES == t
            ]
            if near:
                inside = ((lane - (b + near[0])) & (LANES - 1)) < len(near)
                kept[b % classes] = jnp.where(inside, turn(tile_of(t), b - place), kept[b % classes])

    def straight(start):
        t, skip = divmod(start, LANES)
        value = turn(tile_of(t), -skip)
        if skip + width > LANES:
            value = jnp.where(lane < LANES - skip, value, turn(tile_of(t + 1), -skip))
        return jnp.where(lane < width, value, 0.0)

    west, east = [], []
    for d in range(depth):
        w, e = zero, zero
        for c in range(classes):
            w = jnp.where(lane % classes == c, turn(kept[c], -d), w)
            e = jnp.where((lane + 1) % classes == c, turn(kept[c], d), e)
        west.append(jnp.where(lane < width, w, 0.0))
        east.append(jnp.where(lane < width, e, 0.0))
    south = [straight(d * width) for d in range(depth)]
    north = [straight(cells - (d + 1) * width) for d in range(depth)]
    return west, east, south, north


def slope(value):
    return turn(value, -1) - turn(value, 1)


def place_of(side):
    return (0, 3, 1, 2)[side]


def pack_kernel(width, thick_ref, field_hbm, wet_hbm, diag_hbm, pack_ref, field_ref, wet_ref, diag_ref, tail_ref, flat_ref, lines_ref, sems):
    slots, fields, levels, cells = field_hbm.shape
    pair = 2 * levels
    copies = [pltpu.make_async_copy(wet_hbm, wet_ref, sems.at[0]), pltpu.make_async_copy(diag_hbm, diag_ref, sems.at[1])]
    copies += [pltpu.make_async_copy(field_hbm.at[k], field_ref.at[k], sems.at[2 + k]) for k in range(slots)]
    for copy in copies:
        copy.start()
    copies[0].wait()
    copies[1].wait()
    tiles = tile_count(cells)
    last = tiles - 1
    keep = tile_lanes(cells, last)
    base = fields * levels
    rows = rows_of(pair)
    weights = []
    for start in (0, levels):
        weight = jnp.zeros((pair, LANES), F32)
        for l in range(levels):
            weight = jnp.where(rows == start + l, 0.5 * thick_ref[l], weight)
        weights.append(weight)
    flat_ref[:, last * LANES :] = jnp.zeros((flat_ref.shape[0], LANES), F32)
    if flat_ref.shape[0] > 2 * slots:
        flat_ref[2 * slots :, :] = jnp.zeros((flat_ref.shape[0] - 2 * slots, tiles * LANES), F32)
    for t in range(tiles):
        at = slice(t * LANES, t * LANES + tile_lanes(cells, t))
        for k in range(slots):
            flat_ref[k : k + 1, at] = wet_ref[k, :, at].astype(F32)
            flat_ref[slots + k : slots + k + 1, at] = diag_ref[k, :, at]
    wet = side_lines(lambda t: flat_ref[:, t * LANES : (t + 1) * LANES], flat_ref.shape[0], width, 3)
    tail_ref[...] = jnp.zeros_like(tail_ref)
    lines_ref[...] = jnp.zeros_like(lines_ref)

    def piece(k, f, t):
        if t < last:
            return field_ref[k, f, :, t * LANES : (t + 1) * LANES]
        return tail_ref[k, f]

    def joined(first, second):
        made = {}

        def tile_of(t):
            if t not in made:
                made.clear()
                made[t] = jnp.concatenate([piece(*first, t), piece(*second, t)], axis=0)
            return made[t]

        return tile_of

    for k in range(slots):
        copies[2 + k].wait()
        for f in range(fields):
            tail_ref[k, f, :, :keep] = field_ref[k, f, :, last * LANES : cells]
        both = side_lines(joined((k, 0), (k, 1)), pair, width, 3)
        for e in range(4):
            at = place_of(e) * slots + k
            mask = [wet[e][d][k : k + 1] for d in range(3)]
            pack_ref[at, :pair, :] = both[e][0] * mask[0]
            normal, along = weights if e < 2 else weights[::-1]
            line = slice(e * SUBLANES + k, e * SUBLANES + k + 1)
            for n, (weight, d) in enumerate(((normal, 0), (normal, 1), (normal, 2), (along, 0), (along, 1))):
                lines_ref[n, line, :] = jnp.sum(both[e][d] * weight, axis=0, keepdims=True) * mask[d]
            lines_ref[5, line, :] = mask[0]
            lines_ref[6, line, :] = mask[1]
    normal1, normal2, normal3, along1, along2, wet1, wet2 = (lines_ref[n] for n in range(7))
    inward = jnp.where((rows_of(4 * SUBLANES) // SUBLANES) % 2 == 0, 1.0, -1.0)
    first = wet1 * (inward * normal2 + slope(along1))
    second = wet2 * (inward * (normal3 - normal1) + slope(along2))
    for e in range(4):
        for k in range(slots):
            at = place_of(e) * slots + k
            line = slice(e * SUBLANES + k, e * SUBLANES + k + 1)
            extra = (wet1[line], wet[e][0][slots + k : slots + k + 1], first[line], second[line])
            for n, value in enumerate(extra):
                pack_ref[at, base + n : base + n + 1, :] = value
    scalars = [(k, f) for k in range(slots) for f in range(2, fields)]
    for n in range(0, len(scalars), 2):
        two = scalars[n : n + 2]
        lines = side_lines(joined(two[0], two[-1]), pair, width, 1)
        for m, (k, f) in enumerate(two):
            for e in range(4):
                value = lines[e][0][m * levels : (m + 1) * levels] * wet[e][0][k : k + 1]
                pack_ref[place_of(e) * slots + k, f * levels : (f + 1) * levels, :] = value


def to_rows(flat_ref, out_ref, width, slots, masked):
    lane = lanes_of(SUBLANES)
    count = out_ref.shape[0]

    def one(i):
        t, skip = divmod(i * width, LANES)
        row = turn(flat_ref[:, t * LANES : (t + 1) * LANES], -skip)
        if skip + width > LANES:
            rest = turn(flat_ref[:, (t + 1) * LANES : (t + 2) * LANES], -skip)
            row = jnp.where(lane < LANES - skip, row, rest)
        return row

    for i in range(count):
        row = one(i)
        if count < width:
            row = row + lifted(one(i + count), slots)
        if masked:
            row = jnp.where(lane < width, row, 0.0)
        out_ref[i] = row


def prepare_kernel(width, slots, thick_ref, field_ref, wet_ref, diag_ref, u_ref, v_ref, wet_rows_ref, diag_rows_ref, flat_ref):
    _, _, levels, cells = field_ref.shape
    slot = pl.program_id(0)
    rows = rows_of(levels)
    weight = jnp.zeros((levels, LANES), F32)
    for l in range(levels):
        weight = jnp.where(rows == l, 0.5 * thick_ref[l], weight)

    @pl.when(slot == 0)
    def _():
        flat_ref[...] = jnp.zeros_like(flat_ref)

    for t in range(tile_count(cells)):
        keep = tile_lanes(cells, t)
        at = slice(t * LANES, t * LANES + keep)
        wet = wet_ref[0, :, at].astype(F32)
        factor = weight[:, :keep] * wet
        terms = (
            jnp.sum(field_ref[0, 0, :, at] * factor, axis=0, keepdims=True),
            jnp.sum(field_ref[0, 1, :, at] * factor, axis=0, keepdims=True),
            wet,
            diag_ref[0, :, at],
        )
        mine = rows_of(SUBLANES)[:, :keep] == slot
        for n, term in enumerate(terms):
            flat_ref[n, :, at] = jnp.where(mine, term, flat_ref[n, :, at])

    @pl.when(slot == slots - 1)
    def _():
        to_rows(flat_ref.at[0], u_ref, width, slots, False)
        to_rows(flat_ref.at[1], v_ref, width, slots, False)
        to_rows(flat_ref.at[2], wet_rows_ref, width, slots, True)
        to_rows(flat_ref.at[3], diag_rows_ref, width, slots, False)


def strip_place(shift, strips):
    return jnp.bitwise_and(shift, 1) if strips == 2 else jnp.where(shift < 0, 2, shift)


def partner_block(links_ref, k, e, strips, slots, up_ref, down_ref, beside_ref):
    group_shift = links_ref[k, e, 0]
    place = strip_place(links_ref[k, e, 1], strips)
    partner = jnp.maximum(links_ref[k, e, 2], 0)
    strip = jnp.maximum(place - 1, 0)
    whole = 4 * slots
    most = whole - slots
    entry = place_of(e ^ 1) * slots + partner
    from_up = slots + strip * most + entry - slots
    from_down = slots + strip * most + entry
    if e == 0:
        return up_ref[jnp.where(place == 0, partner, from_up)]
    if e == 1:
        return down_ref[jnp.where(place == 0, partner, from_down)]
    upper = (group_shift < 0).astype(F32)
    lower = (group_shift > 0).astype(F32)
    middle = 1.0 - upper - lower
    return upper * up_ref[from_up] + lower * down_ref[from_down] + middle * beside_ref[strip * whole + entry]


def seam_numbers(links_ref, k, e):
    code = links_ref[k, e, 3]
    live = (links_ref[k, e, 2] >= 0).astype(F32)
    cosine = (code == 0).astype(F32) - (code == 2).astype(F32)
    sine = (code == 1).astype(F32) - (code == 3).astype(F32)
    return (code != 0).astype(jnp.int32), live, cosine, sine


def backward_step(lane, width):
    return jnp.where(lane < width, width - 1 - 2 * lane, 0)


def side_columns(lines_ref, width, slots, fold):
    lane = lanes_of(SUBLANES)
    west = lines_ref[0:SUBLANES, :]
    east = lines_ref[SUBLANES : 2 * SUBLANES, :]
    upper = west, east
    west, east = west, turn(east, width - 1)
    if fold > 1:
        half = width // fold
        west = west + lifted(turn(upper[0], -half), slots)
        east = east + lifted(turn(upper[1], width - 1 - half), slots)

    def column(i):
        return turn(jnp.where(lane == i, west, east), -i)

    return column


def dotted(a_ref, b_ref, chunk=9):
    total = None
    width = a_ref.shape[0]
    for start in range(0, width, chunk):
        part = None
        for i in range(start, min(start + chunk, width)):
            term = a_ref[i] * b_ref[i]
            part = term if part is None else part + term
        total = part if total is None else total + part
    return jnp.sum(total, axis=(0, 1), keepdims=True)


def lines_kernel(width, strips, links_ref, thick_ref, spread_ref, up_ref, down_ref, beside_ref, own_ref,
                 rims_ref, kept_ref, table_ref, lines_ref, numbers_ref):
    slots = links_ref.shape[0]
    fields, levels = spread_ref.shape
    depth = up_ref.shape[1]
    pair = 2 * levels
    base = fields * levels
    lane_all = lanes_of(depth)
    mirror = backward_step(lane_all, width)
    rows = rows_of(pair)
    sign = jnp.where(rows < levels, 1.0, -1.0)
    weights = []
    for start in (0, levels):
        weight = jnp.zeros((pair, LANES), F32)
        for l in range(levels):
            weight = jnp.where(rows == start + l, 0.5 * thick_ref[l], weight)
        weights.append(weight)
    places = 2 if strips == 2 else 3
    lane1 = lanes_of(1)
    lines_ref[...] = jnp.zeros_like(lines_ref)
    numbers_ref[...] = jnp.zeros_like(numbers_ref)
    code_ref = table_ref
    spreads = field_levels(spread_ref, rims_ref.shape[1])
    table = jnp.full((1, LANES), -1, jnp.int32)
    ends = [(e, k) for e in range(4) for k in range(slots)]
    numbers = {at: seam_numbers(links_ref, at[1], at[0]) for at in ends}
    blocks = {at: partner_block(links_ref, at[1], at[0], strips, slots, up_ref, down_ref, beside_ref) for at in ends}
    for at in ends:
        flip, live, _, _ = numbers[at]
        blocks[at] = take_lanes(blocks[at], lane_all + flip * mirror) * live

    def summed(value, weight):
        return jnp.sum(value * weight, axis=0, keepdims=True)

    for at in ends:
        e, k = at
        flip, live, cosine, sine = numbers[at]
        block = blocks[at]
        both = block[:pair]
        turned = cosine * both + (sine * sign) * pltpu.roll(both, levels, 0)
        side = e * slots + k
        mine = place_of(e) * slots + k
        here = own_ref[mine, base : base + 1, :]
        rims_ref[side, :pair] = turned * spreads[:pair] * here
        rims_ref[side, pair:base] = block[pair:base] * spreads[pair:base] * here
        rims_ref[side, base:] = jnp.zeros((rims_ref.shape[1] - base, LANES), F32)
        line = slice(e * SUBLANES + k, e * SUBLANES + k + 1)
        for n in range(4):
            lines_ref[n, line, :] = block[base + n : base + n + 1]
        normal, along = weights if e < 2 else weights[::-1]
        inner = own_ref[mine, :pair, :]
        lines_ref[4, line, :] = summed(both, normal)
        lines_ref[5, line, :] = summed(both, along)
        lines_ref[6, line, :] = summed(inner, normal)
        lines_ref[7, line, :] = summed(inner, along)
        lines_ref[8, line, :] = here
        lines_ref[9, line, :] = own_ref[mine, base + 2 : base + 3, :]
        numbers_ref[0, line, :] = jnp.full((1, LANES), cosine, F32)
        numbers_ref[1, line, :] = jnp.full((1, LANES), sine if e < 2 else -sine, F32)
        partner = links_ref[k, e, 2]
        near = (links_ref[k, e, 0] + 1) * places + strip_place(links_ref[k, e, 1], strips)
        for end in range(2):
            from_lane = partner * ENDS + (e ^ 1) * 2 + (end + flip - 2 * end * flip)
            entry = jnp.where(partner >= 0, near * 32 + from_lane, -1)
            table = jnp.where(lane1 == k * ENDS + e * 2 + end, entry, table)

    wet1, diag1, first, second, normal1, along1, normal0, along0, wet0, own = (lines_ref[n] for n in range(10))
    cosine, sine = numbers_ref[0], numbers_ref[1]
    received = cosine * normal1 + sine * along1
    given = cosine * normal0 - sine * along0
    outward = jnp.where((rows_of(4 * SUBLANES) // SUBLANES) % 2 == 0, 1.0, -1.0)
    first = first + wet1 * (outward * given)
    lane8 = lanes_of(SUBLANES)

    def at_ends(e):
        low, high = (2, 3) if e < 2 else (0, 1)
        place = jnp.full((SUBLANES, LANES), (e % 2) * (width - 1), jnp.int32)
        before = take_lanes(received[low * SUBLANES : (low + 1) * SUBLANES], place)
        after = take_lanes(received[high * SUBLANES : (high + 1) * SUBLANES], place)
        return jnp.where(lane8 == 0, -before, jnp.where(lane8 == width - 1, after, 0.0))

    lateral = jnp.concatenate([at_ends(e) for e in range(4)], axis=0)
    own = own + wet0 * (lateral - outward * received)
    beside = second + own + turn(first, 1) + turn(first, -1)
    far = wet1 * ((4.0 + diag1) * first - beside)
    for n, value in enumerate((received, first, far, wet1)):
        kept_ref[n] = value
    code_ref[...] = table


def source_kernel(width, slots, kept_ref, u_ref, v_ref, wet_ref, r_ref):
    lane = lanes_of(SUBLANES)
    fold = width // r_ref.shape[0]
    column = side_columns(kept_ref.at[0], width, slots, fold)
    south_line = kept_ref[0, 2 * SUBLANES : 3 * SUBLANES, :]
    north_line = kept_ref[0, 3 * SUBLANES : 4 * SUBLANES, :]
    for i in range(r_ref.shape[0]):
        across = u_ref[i]
        cells = column(i)
        west = jnp.where(lane == 0, cells, turn(across, 1))
        east = jnp.where(lane == width - 1, cells, turn(across, -1))
        south = row_south(v_ref, south_line, i, slots, fold)
        north = row_north(v_ref, north_line, i, slots, fold)
        r_ref[i] = wet_ref[i] * (east - west + north - south)


def operator_kernel(width, slots, line, x_ref, kept_ref, diag_ref, wet_ref, out_ref):
    lane = lanes_of(SUBLANES)
    fold = width // x_ref.shape[0]
    column = side_columns(kept_ref.at[line], width, slots, fold)
    south_line = kept_ref[line, 2 * SUBLANES : 3 * SUBLANES, :]
    north_line = kept_ref[line, 3 * SUBLANES : 4 * SUBLANES, :]
    for i in range(x_ref.shape[0]):
        x = x_ref[i]
        ends = column(i)
        west = jnp.where(lane == 0, ends, turn(x, 1))
        east = jnp.where(lane == width - 1, ends, turn(x, -1))
        south = row_south(x_ref, south_line, i, slots, fold)
        north = row_north(x_ref, north_line, i, slots, fold)
        out_ref[i] = wet_ref[i] * ((4.0 + diag_ref[i]) * x - (west + east + south + north))


def totals_kernel(width, slots, kept_ref, table_ref, r_ref, q_ref, w_ref, wet_ref, diag_ref, rows_ref, near_ref):
    stride = slots * ENDS
    lane1 = lanes_of(1)
    lane = lanes_of(SUBLANES)
    first, far, wet1 = kept_ref[1], kept_ref[2], kept_ref[3]
    table = table_ref[...]
    block_of = rows_of(SUBLANES) == lane // ENDS
    which = lane % ENDS
    side = which // 2
    end = which % 2
    upright = side < 2
    column = jnp.where(upright, side, end) * (width - 1)
    upper = jnp.where(upright, end, side - 2) == 1
    step = 1 + end * (width - 3)
    beside_column = jnp.where(upright, column, step)

    def in_row(value):
        value = jnp.sum(jnp.where(block_of, value, 0.0), axis=0, keepdims=True)
        return jnp.where(lane1 < stride, value, 0.0)

    def corners(ref):
        return in_row(jnp.where(upper, take_lanes(row_at(ref, width - 1, slots), column), take_lanes(ref[0], column)))

    def of_lines(value, index):
        total = jnp.zeros((SUBLANES, LANES), F32)
        for e in range(4):
            total = jnp.where(side == e, take_lanes(value[e * SUBLANES : (e + 1) * SUBLANES], index), total)
        return in_row(total)

    lower_row = jnp.where(upright, take_lanes(row_at(q_ref, 1, slots), beside_column), take_lanes(q_ref[0], beside_column))
    upper_row = jnp.where(upright, take_lanes(row_at(q_ref, width - 2, slots), beside_column), take_lanes(row_at(q_ref, width - 1, slots), beside_column))
    q_next = in_row(jnp.where(upper, upper_row, lower_row))
    q_corner = corners(q_ref)
    near = of_lines(wet1, step)
    near_ref[...] = near
    sums = (dotted(r_ref, r_ref), dotted(r_ref, q_ref), dotted(q_ref, q_ref), dotted(q_ref, w_ref))
    total = jnp.zeros((1, LANES), F32)
    for n, value in enumerate(sums):
        total = jnp.where(lane1 == n, value, total)
    last = end * (width - 1)
    code = jnp.where(lane1 < stride, table, 0).astype(F32)
    diag_corner = corners(diag_ref)
    made = []
    for values in (
        (corners(r_ref), of_lines(first, last), q_corner, of_lines(far, last), code),
        (corners(wet_ref), q_next * near - corners(w_ref), q_next, 4.0 + diag_corner, total),
    ):
        row = jnp.zeros((1, LANES), F32)
        for m, value in enumerate(values):
            row = jnp.where((lane1 >= m * stride) & (lane1 < (m + 1) * stride), turn(value, m * stride), row)
        made.append(row)
    both = jnp.where(rows_of(SUBLANES) % 2 == 0, made[0], made[1])
    for start in range(0, rows_ref.shape[0], SUBLANES):
        rows_ref[start : start + SUBLANES, :] = both


def finish_kernel(width, groups, strips, tables_ref, near_ref, r_ref, q_ref, w_ref, wet_ref, x_ref, res_ref, sol_rows, res_rows):
    devices = groups * strips
    slots, _, cells = x_ref.shape
    stride = slots * ENDS
    lane = lanes_of(devices)
    row = rows_of(devices)
    me = lax.axis_index("tiles") * strips + lax.axis_index("strip")
    strip = row % strips
    tables = [tables_ref[pl.ds(n, devices, stride=2), :] for n in range(2)]
    listed = lane < stride

    def part(n, m):
        return jnp.where(listed, turn(tables[n], -m * stride), 0.0)

    r_corner, first_seen, q_seen, far_seen, code = (part(0, m) for m in range(5))
    wet_corner, mixed, q_next, diag_corner, totals = (part(1, m) for m in range(5))
    link = jnp.where(listed, code, -1.0).astype(jnp.int32)
    near = jnp.where(link < 0, -1, link // 32)
    from_lane = jnp.where(link < 0, 0, link % 32)

    def by_rows(value, shift):
        shift %= devices
        return value if shift == 0 else pltpu.roll(value, shift, 0)

    shifts = (0, 1) if strips == 2 else (0, 1, -1)

    def from_partner(value):
        found = jnp.zeros_like(value)
        for group_shift in (-1, 0, 1):
            shifted = by_rows(value, -group_shift * strips)
            for place, strip_shift in enumerate(shifts):
                if group_shift == 0 and strip_shift == 0:
                    continue
                if strip_shift == 0:
                    there = shifted
                elif strip_shift == 1:
                    there = jnp.where(strip < strips - 1, by_rows(shifted, -1), by_rows(shifted, strips - 1))
                else:
                    there = jnp.where(strip > 0, by_rows(shifted, 1), by_rows(shifted, 1 - strips))
                taken = take_lanes(there, from_lane)
                found = jnp.where(near == (group_shift + 1) * len(shifts) + place, taken, found)
        return found

    rise = jnp.where(near >= 0, from_partner(r_corner) - first_seen, 0.0)
    which = lane % ENDS
    other = lane - which + (1 - which // 4) * 4 + (which % 2) * 2 + (which // 2) % 2
    at_corner = rise + take_lanes(rise, other)
    change = -wet_corner * at_corner
    q_corner = q_seen + change
    excess = jnp.where(near >= 0, from_partner(q_corner) - far_seen, 0.0)

    def overall(value):
        return jnp.sum(value, axis=(0, 1), keepdims=True)

    sums = jnp.sum(totals, axis=0, keepdims=True)
    lane1 = lanes_of(1)
    rr, rq, qq, qw = (jnp.sum(jnp.where(lane1 == n, sums, 0.0), axis=1, keepdims=True) for n in range(4))
    rq = rq - overall(r_corner * rise)
    qq = qq + overall(0.5 * wet_corner * at_corner * at_corner - 2.0 * q_seen * rise)
    qw = qw + overall(rise * mixed + q_corner * (0.5 * diag_corner * change - excess) - q_next * change)
    alpha = rr / rq
    next_rr = rr - 2.0 * alpha * rq + alpha * alpha * qq
    image = rq - 2.0 * alpha * qq + alpha * alpha * qw
    ratio = next_rr / rr
    second = next_rr / (image - ratio * next_rr / alpha)

    lane8 = lanes_of(SUBLANES)
    row8 = rows_of(SUBLANES)
    slot8 = row8 * ENDS

    def own(value):
        value = jnp.sum(jnp.where(row == me, value, 0.0), axis=0, keepdims=True)
        return jnp.broadcast_to(value, (SUBLANES, LANES))

    own_change = own(change)
    at_corners = own(0.5 * diag_corner * change - excess)
    at_next = jnp.broadcast_to(near_ref[...], (SUBLANES, LANES)) * own(rise) - own_change

    def entry(value, n):
        return take_lanes(value, slot8 + n)

    def placed(values):
        total = jnp.zeros((SUBLANES, LANES), F32)
        for at, value in values:
            total = jnp.where(lane8 == at, value, total)
        return total

    w_change = {
        0: ((0, entry(at_corners, 0) + entry(at_corners, 4)), (width - 1, entry(at_corners, 2) + entry(at_corners, 5)),
            (1, entry(at_next, 4)), (width - 2, entry(at_next, 5))),
        1: ((0, entry(at_next, 0)), (width - 1, entry(at_next, 2))),
        width - 2: ((0, entry(at_next, 1)), (width - 1, entry(at_next, 3))),
        width - 1: ((0, entry(at_corners, 1) + entry(at_corners, 6)), (width - 1, entry(at_corners, 3) + entry(at_corners, 7)),
                    (1, entry(at_next, 6)), (width - 2, entry(at_next, 7))),
    }
    q_change = {
        0: ((0, entry(own_change, 0)), (width - 1, entry(own_change, 2))),
        width - 1: ((0, entry(own_change, 1)), (width - 1, entry(own_change, 3))),
    }
    count = r_ref.shape[0]

    def corrected(changes, i):
        total = placed(changes[i]) if i in changes else None
        if count < width and i + count in changes:
            upper = lifted(placed(changes[i + count]), slots)
            total = upper if total is None else total + upper
        return total

    for i in range(count):
        r = r_ref[i]
        q = q_ref[i]
        w = w_ref[i]
        q_more, w_more = corrected(q_change, i), corrected(w_change, i)
        if q_more is not None:
            q = q + q_more
        if w_more is not None:
            w = w + wet_ref[i] * w_more
        residual = r - alpha * q
        direction = residual + ratio * r
        sol_rows[i] = alpha * r + second * direction
        res_rows[i] = residual - second * (q - alpha * w + ratio * q)
    for rows_from, out_ref in ((sol_rows, x_ref), (res_rows, res_ref)):
        for t in range(tile_count(cells)):
            keep = tile_lanes(cells, t)
            members = range(t * LANES // width, (t * LANES + keep - 1) // width + 1)
            high = members[0] >= count
            value = None
            for i in members:
                start = i * width - t * LANES
                piece = turn(rows_from[i - count] if high else row_at(rows_from, i, slots), start)
                value = piece if value is None else jnp.where(lane8 >= start, piece, value)
            for k in range(slots):
                line = slots + k if high else k
                out_ref[k, :, t * LANES : t * LANES + keep] = value[line : line + 1, :keep]


def field_levels(spread_ref, count):
    fields, levels = spread_ref.shape
    rows = rows_of(count)
    value = jnp.zeros((count, LANES), F32)
    for f in range(fields):
        for l in range(levels):
            value = jnp.where(rows == f * levels + l, spread_ref[f, l], value)
    return value


def slab_kernel(width, spread_ref, mixing_ref, field_ref, wet_ref, rims_ref, out_ref, masked_ref, wet_row_ref):
    _, fields, levels, cells = field_ref.shape
    count = masked_ref.shape[0]
    tiles = tile_count(cells)
    lane = lanes_of(SUBLANES)
    level = rows_of(SUBLANES) % levels
    tail = tiles - 1
    masked_ref[:, tail * LANES :] = jnp.zeros((count, LANES), F32)
    if count > fields * levels:
        masked_ref[fields * levels :, :] = jnp.zeros((count - fields * levels, tiles * LANES), F32)
    wet_row_ref[:, tail * LANES :] = jnp.zeros((1, LANES), F32)
    for t in range(tiles):
        at = slice(t * LANES, t * LANES + tile_lanes(cells, t))
        wet = wet_ref[0, :, at].astype(F32)
        wet_row_ref[:, at] = wet
        for f in range(fields):
            masked_ref[f * levels : (f + 1) * levels, at] = field_ref[0, f, :, at] * wet
    spreads = field_levels(spread_ref, count)
    mixing = jnp.zeros((SUBLANES, LANES), F32)
    for l in range(levels):
        mixing = jnp.where(level == l, mixing_ref[l], mixing)
    per = SUBLANES // levels
    first = cells - width
    corner, skip = divmod(first, LANES)
    zero = jnp.zeros((SUBLANES, LANES), F32)
    for start in range(0, count, SUBLANES):
        spread = spreads[start : start + SUBLANES]
        west_rim, east_rim, south_rim, north_rim = (rims_ref[e, 0, start : start + SUBLANES, :] for e in range(4))
        north_rim = turn(north_rim, first)

        def tile(t):
            if t < 0 or t >= tiles:
                return zero
            return masked_ref[start : start + SUBLANES, t * LANES : (t + 1) * LANES]

        for t in range(tiles):
            keep = tile_lanes(cells, t)
            value = tile(t)
            west = jnp.where(lane == 0, turn(tile(t - 1), 1), turn(value, 1))
            east = jnp.where(lane == LANES - 1, turn(tile(t + 1), -1), turn(value, -1))
            south = jnp.where(lane < width, turn(tile(t - 1), width), turn(value, width))
            north = jnp.where(lane < LANES - width, turn(value, -width), turn(tile(t + 1), -width))
            added = zero
            for b, at, is_west, is_east in seams(width, t):
                line = zero
                if is_west:
                    west = jnp.where(lane == at % LANES, 0.0, west)
                    line = jnp.where(lane == b, west_rim, line)
                if is_east:
                    east = jnp.where(lane == (at - 1) % LANES, 0.0, east)
                    line = jnp.where(lane == b - 1, east_rim, line)
                added = added + turn(line, at - b)
            if t == 0:
                added = added + south_rim
            if t == corner:
                added = added + jnp.where(lane >= skip, north_rim, 0.0)
            if t == corner + 1:
                added = added + jnp.where(lane < skip, north_rim, 0.0)
            flat = west + east + south + north - 4.0 * value
            above = jnp.where(level == levels - 1, value, pltpu.roll(value, SUBLANES - 1, 0))
            below = jnp.where(level == 0, value, pltpu.roll(value, 1, 0))
            updated = value + spread * flat + mixing * (above + below - 2.0 * value)
            updated = wet_row_ref[:, t * LANES : (t + 1) * LANES] * updated + added
            for n in range(per):
                f = start // levels + n
                if f < fields:
                    out_ref[0, f, :, t * LANES : t * LANES + keep] = updated[n * levels : (n + 1) * levels, :keep]


def cost(flops, moved):
    return pl.CostEstimate(flops=flops, bytes_accessed=moved, transcendentals=0)


def exchange(pack, slots, groups, strips):
    def along(value, axis, size, step):
        return lax.ppermute(value, axis, [(i, (i + step) % size) for i in range(size)])

    beside = [along(pack, "strip", strips, -1)]
    if strips > 2:
        beside.append(along(pack, "strip", strips, 1))
    to_up = jnp.concatenate([pack[3 * slots :]] + [b[slots:] for b in beside], axis=0)
    to_down = jnp.concatenate([pack[:slots]] + [b[: 3 * slots] for b in beside], axis=0)
    beside = jnp.concatenate(beside, axis=0) if strips > 2 else beside[0]
    even = lax.axis_index("tiles") % 2 == 0
    far = lax.ppermute(
        jnp.where(even, to_down, to_up), "tiles", [(i, (i + 1 if i % 2 else i - 1) % groups) for i in range(groups)]
    )
    near = lax.ppermute(jnp.where(even, to_up, to_down), "tiles", [(i, i ^ 1) for i in range(groups)])
    return jnp.where(even, far, near), jnp.where(even, near, far), beside


def on_device(groups, strips, fields, wet_land, links, surface_diagonal, spread, mixing, thickness):
    field = fields[0, 0]
    slots, kinds, levels, cells = field.shape
    width = math.isqrt(cells)
    wet = wet_land.reshape(slots, 1, cells)
    diag = surface_diagonal.reshape(slots, 1, cells)
    seam = links[0, 0]
    depth = -(-(kinds * levels + 4) // SUBLANES) * SUBLANES
    bulk = 4 * field.size
    sides = 4 * slots

    def shape(*dims):
        return jax.ShapeDtypeStruct(dims, F32)

    def per_slot(count):
        return pl.BlockSpec((1, count, levels, cells), lambda s: (s, 0, 0, 0))

    line = pl.BlockSpec((1, 1, cells), lambda s: (s, 0, 0))
    half = width // fold_of(width, slots)
    rows = shape(half, SUBLANES, LANES)
    whole_rows = pl.BlockSpec((half, SUBLANES, LANES), lambda s: (0, 0, 0))
    params = pltpu.CompilerParams(vmem_limit_bytes=8 * 1024 * 1024)
    hbm = pl.BlockSpec(memory_space=pltpu.HBM)

    pack = pl.pallas_call(
        functools.partial(pack_kernel, width),
        in_specs=[SMEM, hbm, hbm, hbm],
        out_specs=VMEM,
        out_shape=pltpu.VMEM((sides, depth, LANES), F32),
        scratch_shapes=[pltpu.VMEM(field.shape, F32), pltpu.VMEM(wet.shape, jnp.int32), pltpu.VMEM(wet.shape, F32),
                        pltpu.VMEM((slots, kinds, levels, LANES), F32), pltpu.VMEM((-(-2 * slots // SUBLANES) * SUBLANES, tile_count(cells) * LANES), F32),
                        pltpu.VMEM((7, 4 * SUBLANES, LANES), F32), pltpu.SemaphoreType.DMA((slots + 2,))],
        cost_estimate=cost(bulk, bulk),
        compiler_params=pltpu.CompilerParams(vmem_limit_bytes=58 * 1024 * 1024),
        name="pack_rims",
    )(thickness, field, wet, diag)
    up, down, beside = exchange(pack, slots, groups, strips)

    slab_rows = -(-kinds * levels // SUBLANES) * SUBLANES
    flat_lanes = tile_count(cells) * LANES
    u, v, wet_rows, diag_rows = pl.pallas_call(
        functools.partial(prepare_kernel, width, slots),
        grid=(slots,),
        in_specs=[SMEM, per_slot(2), line, line],
        out_specs=[whole_rows] * 4,
        out_shape=[rows] * 4,
        scratch_shapes=[pltpu.VMEM((4, SUBLANES, flat_lanes), F32)],
        cost_estimate=cost(64 * bulk, bulk),
        compiler_params=params,
        name="prepare_rows",
    )(thickness, field, wet, diag)

    def local(kernel, outs, operands, scalars=0, scratch=()):
        return pl.pallas_call(
            kernel,
            in_specs=[SMEM] * scalars + [VMEM] * (len(operands) - scalars),
            out_specs=[VMEM] * len(outs),
            out_shape=outs,
            scratch_shapes=list(scratch),
            cost_estimate=cost(bulk, bulk),
            compiler_params=params,
        )(*operands)

    rims, kept, links_row = local(
        functools.partial(lines_kernel, width, strips),
        [shape(sides, slab_rows, LANES), shape(4, 4 * SUBLANES, LANES), jax.ShapeDtypeStruct((1, LANES), jnp.int32)],
        [seam, thickness, spread, up, down, beside, pack],
        3,
        [pltpu.VMEM((10, 4 * SUBLANES, LANES), F32), pltpu.VMEM((2, 4 * SUBLANES, LANES), F32)],
    )
    (r,) = local(functools.partial(source_kernel, width, slots), [rows], [kept, u, v, wet_rows])
    (q,) = local(functools.partial(operator_kernel, width, slots, 1), [rows], [r, kept, diag_rows, wet_rows])
    (w,) = local(functools.partial(operator_kernel, width, slots, 2), [rows], [q, kept, diag_rows, wet_rows])
    devices = groups * strips
    table, near = local(
        functools.partial(totals_kernel, width, slots),
        [pltpu.VMEM((2 * devices, LANES), F32), shape(1, LANES)],
        [kept, links_row, r, q, w, wet_rows, diag_rows],
    )
    tables = lax.all_to_all(table.reshape(devices, 2, LANES), ("tiles", "strip"), 0, 0)

    updated = pl.pallas_call(
        functools.partial(slab_kernel, width),
        grid=(slots,),
        in_specs=[SMEM, SMEM, per_slot(kinds), line, pl.BlockSpec((4, 1, slab_rows, LANES), lambda s: (0, s, 0, 0))],
        out_specs=per_slot(kinds),
        out_shape=shape(slots, kinds, levels, cells),
        scratch_shapes=[pltpu.VMEM((slab_rows, flat_lanes), F32), pltpu.VMEM((1, flat_lanes), F32)],
        cost_estimate=cost(64 * bulk, 2 * bulk),
        compiler_params=params,
        name="slab_step",
    )(spread, mixing, field, wet, rims.reshape(4, slots, slab_rows, LANES))

    surface = shape(slots, 1, cells)
    x, res = pl.pallas_call(
        functools.partial(finish_kernel, width, groups, strips),
        in_specs=[VMEM] * 6,
        out_specs=[VMEM] * 2,
        out_shape=[surface, surface],
        scratch_shapes=[pltpu.VMEM((half, SUBLANES, LANES), F32)] * 2,
        cost_estimate=cost(bulk, bulk),
        compiler_params=pltpu.CompilerParams(vmem_limit_bytes=(8 + devices // 64) * 1024 * 1024),
        name="finish",
    )(tables.reshape(2 * devices, LANES), near, r, q, w, wet_rows)
    return updated[None, None], x.reshape(1, 1, slots, cells), res.reshape(1, 1, slots, cells)


def solution(mesh):
    wide = P("tiles", "strip", None, None, None, None)
    flat = P("tiles", "strip", None, None)
    return jax.shard_map(
        functools.partial(on_device, mesh.shape["tiles"], mesh.shape["strip"]),
        mesh=mesh,
        in_specs=(wide, flat, P("tiles", "strip", None, None, None), flat, P(), P(), P()),
        out_specs=(wide, flat, flat),
        check_vma=False,
    )
```
